32 devices in a mesh: replica: 8 (over z, x), tensor: 4 (over y, core).
Axes of the slice: x: 2, y: 2, z: 4, core: 2. Of those that a mesh axis runs over, the one named last changes fastest.
Arguments:
- queries: bfloat16 [512, 8192], P('replica', 'tensor'), may hold values from -18 to 18
- kv_new: bfloat16 [512, 2, 1024], P('replica', None, 'tensor'), may hold values from -7.5 to 7.5
- pool: bfloat16 [192, 128, 2, 1024], P('replica', None, None, 'tensor'), may hold values from -240 to 240
- page_table: int32 [16, 12], P('replica'), may hold values from 0 to 191, as said below
- hist_len: int32 [16], P('replica'), may hold values from 769 to 1536
- o_weight: bfloat16 [8192, 8192], P('tensor'), may hold values from -0.125 to 0.125
Outputs:
- mixed: bfloat16 [512, 8192], P(('replica', 'tensor'))
The draws below stay inside these ranges and needn't reach their ends.
Inputs may be any that keep to these rules, and one draw needn't show every extreme that they name: `page_table`: no two entries are equal. The owner of page id g is the replica group g // 24. Among the live pages (entry j of conversation c with j * 128 < hist_len[c]) of the conversations of one replica group, at most 3 have any one owner, and in every group some owner holds exactly 3 of them.
All inputs are finite; a program needn't handle non-finite values.
Results may differ from the reference program's by a relative error of at most 0.014.
Values may be sent and summed in bfloat16 or wider, within the bound.
A program may use at most 128 MiB of HBM per device.

```python
import math
import jax
import jax.numpy as jnp
from jax import lax

HEADS = 64
KV_HEADS = 8
HD = 128
D = 8192
NEW = 32
CONV_DEV = 2
PAGE = 128
MAXP = 12
SLOT = 3
CONVS = 16
TOKENS = 512
POOL_DEV = 24
POOL_PAGES = 192
N_TENSOR = 4


def draw_pool(key, part):
    base = jax.random.truncated_normal(key, -6.0, 6.0, (POOL_PAGES, PAGE, 2, KV_HEADS * HD), jnp.float32)
    return base.astype(jnp.bfloat16)


def draw_page_table(key, part):
    groups = CONVS // CONV_DEV
    width = groups * SLOT
    shelves = jax.vmap(lambda owner: jax.random.permutation(jax.random.fold_in(key, 5000 + owner), POOL_DEV))(jnp.arange(groups, dtype=jnp.int32))

    def one_group(group):
        sub = jax.random.fold_in(key, group)
        first = jax.random.randint(jax.random.fold_in(sub, 1), (), 0, groups)
        shuffled = jax.random.permutation(jax.random.fold_in(sub, 2), width).astype(jnp.int32)
        owner_of = jnp.arange(width, dtype=jnp.int32) // SLOT
        score = shuffled - width * (owner_of == first).astype(jnp.int32)
        chosen = jnp.argsort(score, stable=True)[:CONV_DEV * MAXP].astype(jnp.int32)
        owners = chosen // SLOT
        within = chosen % SLOT
        shelf = shelves[owners, group * SLOT + within]
        table = (owners * POOL_DEV + shelf).reshape(CONV_DEV, MAXP)
        front = jax.random.permutation(jax.random.fold_in(sub, 3), MAXP // 2)
        table = table.at[:, :MAXP // 2].set(table[:, front])
        turn = jax.random.randint(jax.random.fold_in(sub, 4), (), 0, CONV_DEV)
        return jnp.roll(table, turn, axis=0)
    return jax.vmap(one_group)(jnp.arange(groups, dtype=jnp.int32)).reshape(CONVS, MAXP).astype(jnp.int32)


def set_ends(entries, own_key, smallest, high):
    extent = entries.shape
    index_at = [jax.random.randint(jax.random.fold_in(own_key, axis), (), 0, extent[axis]) for axis in range(len(extent))]
    entries = entries.at[tuple(index_at)].set(smallest)
    longest = extent.index(max(extent))
    index_at[longest] = (index_at[longest] + 1) % extent[longest]
    return entries.at[tuple(index_at)].set(high)


def level_of(stream_key, dims, pieces, least, top_value):
    def one(position, shards_of):
        heights = jax.random.uniform(jax.random.fold_in(jax.random.fold_in(stream_key, 6), position), (shards_of,), jnp.float32, least / len(pieces), top_value / len(pieces))
        return jnp.repeat(jnp.exp(heights), dims[position] // shards_of).reshape((-1,) + (1,) * (len(dims) - position - 1))

    gain = one(*pieces[0])
    for cut in pieces[1:]:
        gain = gain * one(*cut)
    return gain


def normal_values(stream_key, shape, spread, limit, shards=(), kind=jnp.bfloat16):
    loudness = level_of(stream_key, shape, shards, -0.22, 0.18) if shards else 1.0
    values = jax.random.normal(stream_key, shape, jnp.float32) * spread * loudness
    return jnp.minimum(jnp.maximum(values, -limit), limit).astype(kind)


def setup_inputs(seed: int = 0) -> dict:
    arg_keys = jax.random.split(jax.random.key(seed), 7)
    return {
        "queries": normal_values(arg_keys[0], (TOKENS, HEADS * HD), 3.0, 18.0, ((0, 8), (1, 4))),
        "kv_new": normal_values(arg_keys[1], (TOKENS, 2, KV_HEADS * HD), 1.25, 7.5, ((0, 8), (2, 4))),
        "pool": draw_pool(jax.random.fold_in(arg_keys[6], 71), 0),
        "page_table": draw_page_table(jax.random.fold_in(arg_keys[6], 71), 0),
        "hist_len": set_ends(jax.random.randint(arg_keys[4], (CONVS,), MAXP * PAGE // 2 + 1, MAXP * PAGE + 1), jax.random.fold_in(arg_keys[4], 1), MAXP * PAGE // 2 + 1, MAXP * PAGE).astype(jnp.int32),
        "o_weight": normal_values(arg_keys[5], (HEADS * HD, D), (HEADS * HD // 4) ** -0.5, 0.125, ((0, 4),)),
    }


floor_value = -1e+30

def attend_part(asked, keys, values, allowed):
    scores = jnp.einsum('nkgd,tkd->nkgt', asked.astype(jnp.float32), keys.astype(jnp.float32)) / math.sqrt(HD)
    peak = lax.optimization_barrier(jnp.max(jnp.where(allowed, scores, floor_value), axis=-1))
    weights = jnp.where(allowed, jnp.exp(scores - peak[..., None]), 0.0).astype(jnp.bfloat16)
    weights = lax.optimization_barrier(weights).astype(jnp.float32)
    amount = lax.optimization_barrier(jnp.sum(weights, axis=-1))
    summed = jnp.einsum('nkgt,tkd->nkgd', weights, values.astype(jnp.float32))
    return (peak, amount, summed)

def merge(first, second):
    peak = jnp.maximum(first[0], second[0])
    keep = jnp.exp(first[0] - peak)
    take = jnp.exp(second[0] - peak)
    return (peak, keep * first[1] + take * second[1], keep[..., None] * first[2] + take[..., None] * second[2])

def reference(queries, kv_new, pool, page_table, hist_len, o_weight):
    per_group = HEADS // KV_HEADS
    asked_all = queries.reshape(CONVS, NEW, KV_HEADS, per_group, HD)
    fresh_all = kv_new.reshape(CONVS, NEW, 2, KV_HEADS, HD)
    pool_all = pool.reshape(POOL_PAGES, PAGE, 2, KV_HEADS, HD)
    order = jnp.arange(NEW, dtype=jnp.int32)
    causal = (order[None, :] <= order[:, None])[:, None, None, :]
    inside = jnp.arange(PAGE, dtype=jnp.int32)

    def one_dialog(items):
        asked, fresh, table, length = items
        state = attend_part(asked, fresh[:, 0], fresh[:, 1], causal)

        def step(carry, index):
            page = pool_all[table[index]]
            live = index * PAGE + inside < length
            part = attend_part(asked, page[:, 0], page[:, 1], live[None, None, None, :])
            used = index * PAGE < length
            merged = merge(carry, part)
            return (jax.tree.map(lambda fresh_value, old_value: jnp.where(used, fresh_value, old_value), merged, carry), None)
        state, _ = lax.scan(step, state, jnp.arange(MAXP, dtype=jnp.int32))
        attended = (state[2] / state[1][..., None]).astype(jnp.bfloat16)
        return attended.reshape(NEW, HEADS * HD)
    attended = lax.map(one_dialog, (asked_all, fresh_all, page_table, hist_len)).reshape(TOKENS, N_TENSOR, HEADS * HD // N_TENSOR)
    blocks = o_weight.reshape(N_TENSOR, HEADS * HD // N_TENSOR, D)

    def add_block(running, index):
        part = jnp.dot(attended[:, index], blocks[index], preferred_element_type=jnp.float32)
        part = lax.optimization_barrier(part.astype(jnp.bfloat16)).astype(jnp.float32)
        return (running + part, None)
    running, _ = lax.scan(add_block, jnp.zeros((TOKENS, D), jnp.float32), jnp.arange(N_TENSOR, dtype=jnp.int32))
    return running.astype(jnp.bfloat16)
```

```python
import functools
import math

import jax
import jax.numpy as jnp
from jax import lax
from jax.experimental import pallas as pl
from jax.experimental.pallas import tpu as pltpu
from jax.sharding import PartitionSpec as P

HD = 128
PAGE = 128
SLOT = 3
TILE = 1024
CORES = 2

floor_value = -1e30
tiny_value = 1e-30

MESH = pl.DeviceIdType.MESH
CONTRACT = (((1,), (1,)), ((), ()))


def spread(groups):
    outer = 1
    while outer * outer < groups:
        outer *= 2
    return outer, groups // outer


def selection(rows, kv_count):
    kinds = 2 * kv_count
    tokens = rows // kinds
    i = lax.broadcasted_iota(jnp.int32, (rows, rows), 0)
    j = lax.broadcasted_iota(jnp.int32, (rows, rows), 1)
    source = (i % tokens) * kinds + i // tokens
    return jnp.where(source == j, 1.0, 0.0).astype(jnp.bfloat16)


def kernel(
    groups, shards,
    q_hbm, fresh_hbm, pool_hbm, table_hbm, length_hbm, weight,
    out_ref,
    table, length, listed, pool_ref, fresh_ref, outgoing, arrived, wbuf, perm, qall, qcur, kbuf, vbuf,
    peak_ref, amount_ref, summed_ref, back, back_log, came, came_log, attended, part, sibling, joined, landed,
    load_sem, q_load_sem, weight_sem,
    table_send, table_recv, length_send, length_recv,
    q_send, q_recv, page_send, page_recv,
    back_send, back_recv, log_send, log_recv,
    core_send, core_recv, part_send, part_recv,
):
    outer, inner = spread(groups)
    half = outer // 2
    me = lax.axis_index("replica")
    mine = lax.axis_index("tensor")
    z = me // inner
    x = me % inner
    pool_size = pool_ref.shape[0]
    _, kv_count, dialogs, rows, _ = qall.shape
    entries = table.shape[2]
    token_rows = q_hbm.shape[0]
    new_len = token_rows // dialogs
    per_group = rows // new_len
    tiles, _, chips, block_rows, tile = part.shape
    block = perm.shape[0]
    page_rows = pool_ref.shape[1]
    block_tokens = block // (2 * kv_count)
    scale = math.log2(math.e) / math.sqrt(HD)
    chip = mine // CORES
    core = mine % CORES

    loads = [
        pltpu.make_async_copy(table_hbm, table.at[me], load_sem.at[0]),
        pltpu.make_async_copy(length_hbm, length.at[me], load_sem.at[1]),
        pltpu.make_async_copy(pool_hbm, pool_ref, load_sem.at[2]),
        pltpu.make_async_copy(fresh_hbm, fresh_ref, load_sem.at[3]),
    ]

    def q_load(k, d, g):
        col = (k * per_group + g) * HD
        return pltpu.make_async_copy(
            q_hbm.at[d * new_len : (d + 1) * new_len, col : col + HD],
            qall.at[z, k, d, g * new_len : (g + 1) * new_len, :],
            q_load_sem.at[k, d, g],
        )

    q_loads = [
        q_load(k, d, g) for k in range(kv_count) for d in range(dialogs) for g in range(per_group)
    ]

    loads[0].start()
    loads[1].start()
    for copy in q_loads:
        copy.start()
    loads[2].start()
    loads[3].start()

    barrier = pltpu.get_barrier_semaphore()
    for step in range(1, groups):
        pl.semaphore_signal(
            barrier, inc=1, device_id={"replica": lax.rem(me + step, groups)}, device_id_type=MESH
        )
    for step in range(1, shards):
        pl.semaphore_signal(
            barrier, inc=1, device_id={"tensor": lax.rem(mine + step, shards)}, device_id_type=MESH
        )

    def table_copy(step):
        return pltpu.make_async_remote_copy(
            src_ref=table.at[me],
            dst_ref=table.at[me],
            send_sem=table_send.at[step],
            recv_sem=table_recv.at[step],
            device_id={"replica": lax.rem(me + step, groups)},
            device_id_type=MESH,
        )

    def length_copy(step):
        return pltpu.make_async_remote_copy(
            src_ref=length.at[me],
            dst_ref=length.at[me],
            send_sem=length_send.at[step],
            recv_sem=length_recv.at[step],
            device_id={"replica": lax.rem(me + step, groups)},
            device_id_type=MESH,
        )

    def q_copy(group, k, way):
        dest = z + (1 if way == 0 else -1)
        return pltpu.make_async_remote_copy(
            src_ref=qall.at[group, k],
            dst_ref=qall.at[group, k],
            send_sem=q_send.at[way, group, k],
            recv_sem=q_recv.at[group, k],
            device_id={"replica": dest * inner + x},
            device_id_type=MESH,
        )

    def page_copy(step, group):
        return pltpu.make_async_remote_copy(
            src_ref=outgoing.at[step - 1, group],
            dst_ref=arrived.at[step - 1, group],
            send_sem=page_send.at[step - 1, group],
            recv_sem=page_recv.at[step - 1, group],
            device_id={"replica": z * inner + lax.rem(x + step, inner)},
            device_id_type=MESH,
        )

    def back_copy(group):
        return pltpu.make_async_remote_copy(
            src_ref=back.at[group],
            dst_ref=came.at[z],
            send_sem=back_send.at[group],
            recv_sem=back_recv.at[z],
            device_id={"replica": group * inner + x},
            device_id_type=MESH,
        )

    def log_copy(group):
        return pltpu.make_async_remote_copy(
            src_ref=back_log.at[group],
            dst_ref=came_log.at[z],
            send_sem=log_send.at[group],
            recv_sem=log_recv.at[z],
            device_id={"replica": group * inner + x},
            device_id_type=MESH,
        )

    def weight_copy(index):
        return pltpu.make_async_copy(
            weight.at[:, pl.ds(pl.multiple_of(index * tile, tile), tile)],
            wbuf.at[index],
            weight_sem.at[index],
        )

    def core_copy(index):
        return pltpu.make_async_remote_copy(
            src_ref=part.at[index, 1 - core],
            dst_ref=sibling.at[index],
            send_sem=core_send.at[index],
            recv_sem=core_recv.at[index],
            device_id={"tensor": chip * CORES + 1 - core},
            device_id_type=MESH,
        )

    def part_copy(index, step):
        dest = lax.rem(chip + step, chips)
        return pltpu.make_async_remote_copy(
            src_ref=joined.at[index, step - 1],
            dst_ref=landed.at[index, step - 1],
            send_sem=part_send.at[index, step - 1],
            recv_sem=part_recv.at[index, step - 1],
            device_id={"tensor": dest * CORES + core},
            device_id_type=MESH,
        )

    perm[...] = selection(block, kv_count)

    side = z // half

    def served(turn):
        across = (1 - side) * (half + turn) + side * (half - 1 - turn)
        beside = side * half + lax.rem(z - side * half + 1 + turn - half + outer, half)
        far = (turn < half).astype(jnp.int32) if not isinstance(turn, int) else int(turn < half)
        return far * across + (1 - far) * beside

    loads[0].wait()
    loads[1].wait()
    pl.semaphore_wait(barrier, groups + shards - 2)
    for step in range(1, groups):
        table_copy(step).start()
        length_copy(step).start()
    for copy in q_loads:
        copy.wait()
    for k in range(kv_count):
        @pl.when(z < outer - 1)
        def _():
            q_copy(z, k, 0).start()

        @pl.when(z > 0)
        def _():
            q_copy(z, k, 1).start()

    loads[2].wait()
    loads[3].wait()
    for step in range(1, groups):
        table_copy(step).wait_recv()
        length_copy(step).wait_recv()

    def request(group, owner):
        count = jnp.int32(0)
        zero = jnp.int32(0)
        shelf, dialog, fill = [zero] * SLOT, [zero] * SLOT, [zero] * SLOT
        low = owner * pool_size
        for d in range(dialogs):
            total = length[group, d]
            for e in range(entries):
                place = table[group, d, e] - low
                live = jnp.minimum(total - e * PAGE, PAGE)
                hit = (place >= 0) & (place < pool_size) & (live > 0)
                for s in range(SLOT):
                    here = hit & (count == s)
                    shelf[s] = jnp.where(here, place, shelf[s])
                    dialog[s] = jnp.where(here, d, dialog[s])
                    fill[s] = jnp.where(here, live, fill[s])
                count = count + hit.astype(jnp.int32)
        return shelf, dialog, fill

    def send_pages(turn, carry):
        group = served(turn)
        for step in range(1, inner):
            shelf, _, _ = request(group * inner + lax.rem(x + step, inner), me)
            for s in range(SLOT):
                outgoing[step - 1, group, s] = pool_ref[shelf[s]]
            page_copy(step, group).start()
        return carry

    lax.fori_loop(0, outer, send_pages, 0)

    for index in range(tiles):
        weight_copy(index).start()

    def list_pages(group, carry):
        for step in range(inner):
            shelf, dialog, fill = request(
                group * inner + x, z * inner + lax.rem(x - step + inner, inner)
            )
            for s in range(SLOT):
                listed[group, step, s, 0] = shelf[s]
                listed[group, step, s, 1] = dialog[s]
                listed[group, step, s, 2] = fill[s]
        return carry

    lax.fori_loop(0, outer, list_pages, 0)

    fresh_rows = fresh_ref.shape[0]
    split = jnp.dot(
        selection(fresh_rows, kv_count), fresh_ref[...], preferred_element_type=jnp.float32
    ).astype(jnp.bfloat16)
    row_token = lax.broadcasted_iota(jnp.int32, (rows, token_rows), 0) % new_len
    col_token = lax.broadcasted_iota(jnp.int32, (rows, token_rows), 1)
    for k in range(kv_count):
        keys = split[(2 * k) * token_rows : (2 * k + 1) * token_rows]
        values = split[(2 * k + 1) * token_rows : (2 * k + 2) * token_rows]
        for d in range(dialogs):
            scores = lax.dot_general(
                qall[z, k, d], keys, CONTRACT, preferred_element_type=jnp.float32
            ) * scale
            causal = (col_token // new_len == d) & (col_token - d * new_len <= row_token)
            scores = jnp.where(causal, scores, floor_value)
            peak = jnp.max(scores, axis=-1, keepdims=True)
            weights = jnp.exp2(scores - peak).astype(jnp.bfloat16)
            peak_ref[z, k, d] = jnp.broadcast_to(peak, (rows, HD))
            amount_ref[z, k, d] = jnp.broadcast_to(
                jnp.sum(weights.astype(jnp.float32), axis=-1, keepdims=True), (rows, HD)
            )
            summed_ref[z, k, d] = jnp.dot(weights, values, preferred_element_type=jnp.float32)

    def absorb(group, step, fetch, first):
        position = lax.broadcasted_iota(jnp.int32, (rows, PAGE), 1)
        dialog, fill = [], []
        for s in range(SLOT):
            dialog.append(listed[group, step, s, 1])
            fill.append(listed[group, step, s, 2])
            for b in range(page_rows // block):
                split = jnp.dot(
                    perm[...], fetch(s, b), preferred_element_type=jnp.float32
                ).astype(jnp.bfloat16)
                at = s * PAGE + b * block_tokens
                for k in range(kv_count):
                    low = 2 * k * block_tokens
                    kbuf[k, at : at + block_tokens, :] = split[low : low + block_tokens]
                    vbuf[k, at : at + block_tokens, :] = split[
                        low + block_tokens : low + 2 * block_tokens
                    ]
        owned = [
            [jnp.broadcast_to(dialog[s], (rows, HD)) == d for d in range(dialogs)]
            for s in range(SLOT)
        ]
        for k in range(kv_count):
            for d in range(dialogs):
                qcur[k, d] = qall[group, k, d]
            scores, highs = [], []
            for s in range(SLOT):
                keys = kbuf[k, s * PAGE : (s + 1) * PAGE, :]
                found = lax.dot_general(
                    qcur[k, dialog[s]], keys, CONTRACT, preferred_element_type=jnp.float32
                ) * scale
                found = jnp.where(position < fill[s], found, floor_value)
                scores.append(found)
                highs.append(
                    jnp.broadcast_to(jnp.max(found, axis=-1, keepdims=True), (rows, HD))
                )
            peaks, keeps = [], []
            for d in range(dialogs):
                peak = functools.reduce(
                    jnp.maximum,
                    [jnp.where(owned[s][d], highs[s], floor_value) for s in range(SLOT)],
                )
                if not first:
                    before = peak_ref[group, k, d]
                    peak = jnp.maximum(peak, before)
                    keeps.append(jnp.exp2(before - peak))
                peaks.append(peak)
                peak_ref[group, k, d] = peak
            amounts, sums = [], []
            for s in range(SLOT):
                peak = peaks[-1]
                for d in reversed(range(dialogs - 1)):
                    peak = jnp.where(owned[s][d], peaks[d], peak)
                weights = jnp.exp2(scores[s] - peak).astype(jnp.bfloat16)
                values = vbuf[k, s * PAGE : (s + 1) * PAGE, :]
                amounts.append(
                    jnp.broadcast_to(
                        jnp.sum(weights.astype(jnp.float32), axis=-1, keepdims=True), (rows, HD)
                    )
                )
                sums.append(jnp.dot(weights, values, preferred_element_type=jnp.float32))
            for d in range(dialogs):
                amount = functools.reduce(
                    jnp.add, [jnp.where(owned[s][d], amounts[s], 0.0) for s in range(SLOT)]
                )
                total = functools.reduce(
                    jnp.add, [jnp.where(owned[s][d], sums[s], 0.0) for s in range(SLOT)]
                )
                if not first:
                    amount = amount + keeps[d] * amount_ref[group, k, d]
                    total = total + keeps[d] * summed_ref[group, k, d]
                amount_ref[group, k, d] = amount
                summed_ref[group, k, d] = total

    def absorb_own(group, first):
        shelf = [listed[group, 0, s, 0] for s in range(SLOT)]
        absorb(
            group, 0, lambda s, b: pool_ref[shelf[s], b * block : (b + 1) * block, :], first
        )

    def absorb_arrived(group):
        for step in range(1, inner):
            page_copy(step, group).wait_recv()
            absorb(
                group,
                step,
                lambda s, b: arrived[step - 1, group, s, b * block : (b + 1) * block, :],
                False,
            )

    absorb_own(z, False)

    def relay(distance):
        for k in range(kv_count):
            @pl.when(z >= distance)
            def _():
                q_copy(z - distance, k, 0).wait_recv()

            @pl.when((z >= distance) & (z < outer - 1))
            def _():
                q_copy(z - distance, k, 0).start()

            @pl.when(z < outer - distance)
            def _():
                q_copy(z + distance, k, 1).wait_recv()

            @pl.when((z < outer - distance) & (z > 0))
            def _():
                q_copy(z + distance, k, 1).start()

    def serve(turn, carry):
        group = served(turn)
        absorb_own(group, True)
        absorb_arrived(group)
        for k in range(kv_count):
            for d in range(dialogs):
                amount = jnp.maximum(amount_ref[group, k, d], tiny_value)
                back[group, k, d] = (summed_ref[group, k, d] / amount).astype(jnp.bfloat16)
                log = peak_ref[group, k, d] + jnp.log2(amount)
                back_log[group, pl.ds(k * dialogs + d, 1), :] = jnp.transpose(log)[:1]
        back_copy(group).start()
        log_copy(group).start()
        return carry

    for distance in range(1, half + 1):
        relay(distance)
    lax.fori_loop(0, 1, serve, 0)
    for distance in range(half + 1, outer):
        relay(distance)
    lax.fori_loop(1, outer - 1, serve, 0)

    def merge(turn, carry):
        source = served(turn)
        back_copy_in(source)
        for k in range(kv_count):
            for d in range(dialogs):
                line = came_log[source, pl.ds(k * dialogs + d, 1), :]
                log = jnp.transpose(jnp.broadcast_to(line, (HD, rows)))
                before = peak_ref[z, k, d]
                peak = jnp.maximum(before, log)
                keep = jnp.exp2(before - peak)
                take = jnp.exp2(log - peak)
                peak_ref[z, k, d] = peak
                amount_ref[z, k, d] = keep * amount_ref[z, k, d] + take
                summed_ref[z, k, d] = keep * summed_ref[z, k, d] + take * came[
                    source, k, d
                ].astype(jnp.float32)
        return carry

    def back_copy_in(source):
        pltpu.make_async_remote_copy(
            src_ref=back.at[source],
            dst_ref=came.at[source],
            send_sem=back_send.at[source],
            recv_sem=back_recv.at[source],
            device_id={"replica": source * inner + x},
            device_id_type=MESH,
        ).wait_recv()
        pltpu.make_async_remote_copy(
            src_ref=back_log.at[source],
            dst_ref=came_log.at[source],
            send_sem=log_send.at[source],
            recv_sem=log_recv.at[source],
            device_id={"replica": source * inner + x},
            device_id_type=MESH,
        ).wait_recv()

    lax.fori_loop(0, half, merge, 0)
    absorb_arrived(z)
    lax.fori_loop(half, outer - 1, merge, 0)

    for k in range(kv_count):
        for d in range(dialogs):
            ratio = (summed_ref[z, k, d] / amount_ref[z, k, d]).astype(jnp.bfloat16)
            for g in range(per_group):
                col = (k * per_group + g) * HD
                attended[d * new_len : (d + 1) * new_len, col : col + HD] = ratio[
                    g * new_len : (g + 1) * new_len
                ]

    def join(index):
        core_copy(index).wait_recv()
        for step in range(1, chips):
            dest = lax.rem(chip + step, chips)
            total = part[index, core, dest].astype(jnp.float32) + sibling[index, dest].astype(
                jnp.float32
            )
            joined[index, step - 1] = total.astype(jnp.bfloat16)
            part_copy(index, step).start()

    def project(index, carry):
        weight_copy(index).wait()
        product = jnp.dot(attended[...], wbuf[index], preferred_element_type=jnp.float32)
        product = product.astype(jnp.bfloat16)
        for dest in range(shards):
            part[index, dest % CORES, dest // CORES] = product[
                dest * block_rows : (dest + 1) * block_rows
            ]
        core_copy(index).start()

        @pl.when(index > 0)
        def _():
            join(index - 1)

        return carry

    lax.fori_loop(0, tiles, project, 0)
    join(tiles - 1)

    def finish(index, carry):
        total = part[index, core, chip].astype(jnp.float32) + sibling[index, chip].astype(
            jnp.float32
        )
        for step in range(1, chips):
            part_copy(index, step).wait_recv()
            total = total + landed[index, step - 1].astype(jnp.float32)
        out_ref[:, pl.ds(pl.multiple_of(index * tile, tile), tile)] = total.astype(out_ref.dtype)
        return carry

    lax.fori_loop(0, tiles, finish, 0)

    def drain(index, carry):
        core_copy(index).wait_send()
        for step in range(1, chips):
            part_copy(index, step).wait_send()
        return carry

    lax.fori_loop(0, tiles, drain, 0)

    def drain_back(turn, carry):
        back_copy(served(turn)).wait_send()
        log_copy(served(turn)).wait_send()
        return carry

    lax.fori_loop(0, outer - 1, drain_back, 0)

    def drain_line(group, carry):
        for step in range(1, inner):
            page_copy(step, group).wait_send()
        for k in range(kv_count):
            @pl.when((group <= z) & (z < outer - 1))
            def _():
                q_copy(group, k, 0).wait_send()

            @pl.when((group >= z) & (z > 0))
            def _():
                q_copy(group, k, 1).wait_send()

        return carry

    lax.fori_loop(0, outer, drain_line, 0)
    for step in range(1, groups):
        table_copy(step).wait_send()
        length_copy(step).wait_send()


def local(queries, kv_new, pool, page_table, hist_len, o_weight):
    groups = lax.axis_size("replica")
    shards = lax.axis_size("tensor")
    outer, inner = spread(groups)
    pool_size, page_len, _, kv_width = pool.shape
    dialogs, entries = page_table.shape
    token_rows = queries.shape[0]
    new_len = token_rows // dialogs
    kv_count = kv_width // HD
    per_group = queries.shape[1] // kv_width
    rows = per_group * new_len
    depth, model = o_weight.shape
    tile = min(TILE, model)
    tiles = model // tile
    block_rows = token_rows // shards
    chips = shards // CORES
    page_rows = 2 * kv_count * page_len
    block = 256
    pages = pool.reshape(pool_size, page_len, 2, kv_count, HD).transpose(0, 1, 3, 2, 4)
    pages = pages.reshape(pool_size, page_rows, HD)
    fresh = kv_new.reshape(token_rows, 2, kv_count, HD).transpose(0, 2, 1, 3)
    fresh = fresh.reshape(2 * kv_count * token_rows, HD)
    vmem = pl.BlockSpec(memory_space=pltpu.VMEM)
    anywhere = pl.BlockSpec(memory_space=pl.ANY)
    dma = pltpu.SemaphoreType.DMA
    bf16, f32 = jnp.bfloat16, jnp.float32
    return pl.pallas_call(
        functools.partial(kernel, groups, shards),
        out_shape=jax.ShapeDtypeStruct((block_rows, model), jnp.bfloat16),
        in_specs=[anywhere] * 6,
        out_specs=vmem,
        scratch_shapes=[
            pltpu.SMEM((groups, dialogs, entries), jnp.int32),
            pltpu.SMEM((groups, dialogs), jnp.int32),
            pltpu.SMEM((outer, inner, SLOT, 3), jnp.int32),
            pltpu.VMEM((pool_size, page_rows, HD), bf16),
            pltpu.VMEM((2 * kv_count * token_rows, HD), bf16),
            pltpu.VMEM((inner - 1, outer, SLOT, page_rows, HD), bf16),
            pltpu.VMEM((inner - 1, outer, SLOT, page_rows, HD), bf16),
            pltpu.VMEM((tiles, depth, tile), bf16),
            pltpu.VMEM((block, block), bf16),
            pltpu.VMEM((outer, kv_count, dialogs, rows, HD), bf16),
            pltpu.VMEM((kv_count, dialogs, rows, HD), bf16),
            pltpu.VMEM((kv_count, SLOT * page_len, HD), bf16),
            pltpu.VMEM((kv_count, SLOT * page_len, HD), bf16),
            pltpu.VMEM((outer, kv_count, dialogs, rows, HD), f32),
            pltpu.VMEM((outer, kv_count, dialogs, rows, HD), f32),
            pltpu.VMEM((outer, kv_count, dialogs, rows, HD), f32),
            pltpu.VMEM((outer, kv_count, dialogs, rows, HD), bf16),
            pltpu.VMEM((outer, kv_count * dialogs, rows), f32),
            pltpu.VMEM((outer, kv_count, dialogs, rows, HD), bf16),
            pltpu.VMEM((outer, kv_count * dialogs, rows), f32),
            pltpu.VMEM((token_rows, depth), bf16),
            pltpu.VMEM((tiles, CORES, chips, block_rows, tile), bf16),
            pltpu.VMEM((tiles, chips, block_rows, tile), bf16),
            pltpu.VMEM((tiles, chips - 1, block_rows, tile), bf16),
            pltpu.VMEM((tiles, chips - 1, block_rows, tile), bf16),
            dma((4,)),
            dma((kv_count, dialogs, per_group)),
            dma((tiles,)),
            dma((groups,)),
            dma((groups,)),
            dma((groups,)),
            dma((groups,)),
            dma((2, outer, kv_count)),
            dma((outer, kv_count)),
            dma((inner - 1, outer)),
            dma((inner - 1, outer)),
            dma((outer,)),
            dma((outer,)),
            dma((outer,)),
            dma((outer,)),
            dma((tiles,)),
            dma((tiles,)),
            dma((tiles, chips - 1)),
            dma((tiles, chips - 1)),
        ],
        compiler_params=pltpu.CompilerParams(
            collective_id=0, has_side_effects=True, vmem_limit_bytes=63 * 1024 * 1024
        ),
        name="attend",
    )(queries, fresh, pages, page_table, hist_len, o_weight)


def solution(mesh):
    in_specs = (
        P("replica", "tensor"),
        P("replica", None, "tensor"),
        P("replica", None, None, "tensor"),
        P("replica", None),
        P("replica"),
        P("tensor", None),
    )
    out_specs = P(("replica", "tensor"), None)
    return jax.shard_map(local, mesh=mesh, in_specs=in_specs, out_specs=out_specs, check_vma=False)
```

```python
import functools
import math

import jax
import jax.numpy as jnp
from jax import lax
from jax.experimental import pallas as pl
from jax.experimental.pallas import tpu as pltpu
from jax.sharding import PartitionSpec as P

HD = 128
PAGE = 128
SLOT = 3
TILE = 512
LAG = 4
CORES = 2

floor_value = -1e30
tiny_value = 1e-30

MESH = pl.DeviceIdType.MESH
CONTRACT = (((1,), (1,)), ((), ()))


def spread(groups):
    outer = 1
    while outer * outer < groups:
        outer *= 2
    return outer, groups // outer


def selection(rows, kv_count):
    kinds = 2 * kv_count
    tokens = rows // kinds
    i = lax.broadcasted_iota(jnp.int32, (rows, rows), 0)
    j = lax.broadcasted_iota(jnp.int32, (rows, rows), 1)
    source = (i % tokens) * kinds + i // tokens
    return jnp.where(source == j, 1.0, 0.0).astype(jnp.bfloat16)


def kernel(
    groups, shards,
    q_hbm, fresh_hbm, pool_hbm, table_hbm, length_hbm, weight,
    out_ref,
    table, length, listed, pool_ref, fresh_ref, kept, outgoing, arrived, wbuf, perm, qall, qcur,
    peak_ref, amount_ref, summed_ref, back, back_log, came, came_log, attended, gathered,
    part, sibling, joined, landed,
    load_sem, q_load_sem, weight_sem,
    table_send, table_recv, length_send, length_recv,
    q_send, q_recv, page_send, page_recv,
    back_send, back_recv, log_send, log_recv,
    core_send, core_recv, part_send, part_recv,
):
    outer, inner = spread(groups)
    half = outer // 2
    me = lax.axis_index("replica")
    mine = lax.axis_index("tensor")
    z = me // inner
    x = me % inner
    pool_size = pool_ref.shape[0]
    _, kv_count, dialogs, rows, _ = qall.shape
    entries = table.shape[2]
    token_rows = q_hbm.shape[0]
    new_len = token_rows // dialogs
    per_group = rows // new_len
    tiles, _, chips, block_rows, tile = part.shape
    block = perm.shape[0]
    page_rows = pool_ref.shape[1]
    block_tokens = block // (2 * kv_count)
    scale = math.log2(math.e) / math.sqrt(HD)
    chip = mine // CORES
    core = mine % CORES

    loads = [
        pltpu.make_async_copy(table_hbm, table.at[me], load_sem.at[0]),
        pltpu.make_async_copy(length_hbm, length.at[me], load_sem.at[1]),
        pltpu.make_async_copy(pool_hbm, pool_ref, load_sem.at[2]),
        pltpu.make_async_copy(fresh_hbm, fresh_ref, load_sem.at[3]),
    ]

    def q_load(k, d, g):
        col = (k * per_group + g) * HD
        return pltpu.make_async_copy(
            q_hbm.at[d * new_len : (d + 1) * new_len, col : col + HD],
            qall.at[z, k, d, g * new_len : (g + 1) * new_len, :],
            q_load_sem.at[k, d, g],
        )

    q_loads = [
        q_load(k, d, g) for k in range(kv_count) for d in range(dialogs) for g in range(per_group)
    ]

    loads[0].start()
    loads[1].start()
    for copy in q_loads:
        copy.start()
    loads[2].start()
    loads[3].start()

    barrier = pltpu.get_barrier_semaphore()
    for step in range(1, groups):
        pl.semaphore_signal(
            barrier, inc=1, device_id={"replica": lax.rem(me + step, groups)}, device_id_type=MESH
        )
    for step in range(1, shards):
        pl.semaphore_signal(
            barrier, inc=1, device_id={"tensor": lax.rem(mine + step, shards)}, device_id_type=MESH
        )

    def table_copy(step):
        return pltpu.make_async_remote_copy(
            src_ref=table.at[me],
            dst_ref=table.at[me],
            send_sem=table_send.at[step],
            recv_sem=table_recv.at[step],
            device_id={"replica": lax.rem(me + step, groups)},
            device_id_type=MESH,
        )

    def length_copy(step):
        return pltpu.make_async_remote_copy(
            src_ref=length.at[me],
            dst_ref=length.at[me],
            send_sem=length_send.at[step],
            recv_sem=length_recv.at[step],
            device_id={"replica": lax.rem(me + step, groups)},
            device_id_type=MESH,
        )

    def q_copy(group, k, way):
        dest = z + (1 if way == 0 else -1)
        return pltpu.make_async_remote_copy(
            src_ref=qall.at[group, k],
            dst_ref=qall.at[group, k],
            send_sem=q_send.at[way, group, k],
            recv_sem=q_recv.at[group, k],
            device_id={"replica": dest * inner + x},
            device_id_type=MESH,
        )

    def page_copy(step, group, k):
        return pltpu.make_async_remote_copy(
            src_ref=outgoing.at[step - 1, group, k],
            dst_ref=arrived.at[step - 1, group, k],
            send_sem=page_send.at[step - 1, group, k],
            recv_sem=page_recv.at[step - 1, group, k],
            device_id={"replica": z * inner + lax.rem(x + step, inner)},
            device_id_type=MESH,
        )

    def back_copy(group, k, source):
        return pltpu.make_async_remote_copy(
            src_ref=back.at[group, k],
            dst_ref=came.at[source, k],
            send_sem=back_send.at[group, k],
            recv_sem=back_recv.at[source, k],
            device_id={"replica": group * inner + x},
            device_id_type=MESH,
        )

    def log_copy(group, k, source):
        return pltpu.make_async_remote_copy(
            src_ref=back_log.at[group, k],
            dst_ref=came_log.at[source, k],
            send_sem=log_send.at[group, k],
            recv_sem=log_recv.at[source, k],
            device_id={"replica": group * inner + x},
            device_id_type=MESH,
        )

    def weight_copy(index):
        return pltpu.make_async_copy(
            weight.at[:, pl.ds(pl.multiple_of(index * tile, tile), tile)],
            wbuf.at[index],
            weight_sem.at[index],
        )

    def core_copy(index):
        return pltpu.make_async_remote_copy(
            src_ref=part.at[index, 1 - core],
            dst_ref=sibling.at[index],
            send_sem=core_send.at[index],
            recv_sem=core_recv.at[index],
            device_id={"tensor": chip * CORES + 1 - core},
            device_id_type=MESH,
        )

    def part_copy(index, step):
        dest = lax.rem(chip + step, chips)
        return pltpu.make_async_remote_copy(
            src_ref=joined.at[index, step - 1],
            dst_ref=landed.at[index, step - 1],
            send_sem=part_send.at[index, step - 1],
            recv_sem=part_recv.at[index, step - 1],
            device_id={"tensor": dest * CORES + core},
            device_id_type=MESH,
        )

    perm[...] = selection(block, kv_count)

    side = z // half

    def served(turn):
        across = (1 - side) * (half + turn) + side * (half - 1 - turn)
        beside = side * half + lax.rem(z - side * half + 1 + turn - half + outer, half)
        far = (turn < half).astype(jnp.int32) if not isinstance(turn, int) else int(turn < half)
        return far * across + (1 - far) * beside

    loads[0].wait()
    loads[1].wait()
    pl.semaphore_wait(barrier, groups + shards - 2)
    for step in range(1, groups):
        table_copy(step).start()
        length_copy(step).start()
    for copy in q_loads:
        copy.wait()
    for k in range(kv_count):
        @pl.when(z < outer - 1)
        def _():
            q_copy(z, k, 0).start()

        @pl.when(z > 0)
        def _():
            q_copy(z, k, 1).start()

    loads[2].wait()
    loads[3].wait()

    def request(group, owner):
        count = jnp.int32(0)
        zero = jnp.int32(0)
        shelf, dialog, fill = [zero] * SLOT, [zero] * SLOT, [zero] * SLOT
        low = owner * pool_size
        for d in range(dialogs):
            total = length[group, d]
            for e in range(entries):
                place = table[group, d, e] - low
                live = jnp.minimum(total - e * PAGE, PAGE)
                hit = (place >= 0) & (place < pool_size) & (live > 0)
                for s in range(SLOT):
                    here = hit & (count == s)
                    shelf[s] = jnp.where(here, place, shelf[s])
                    dialog[s] = jnp.where(here, d, dialog[s])
                    fill[s] = jnp.where(here, live, fill[s])
                count = count + hit.astype(jnp.int32)
        return shelf, dialog, fill

    def await_tables(group):
        for other in range(inner):
            source = group * inner + other
            step = lax.rem(me - source + groups, groups)

            @pl.when(source != me)
            def _():
                table_copy(step).wait_recv()
                length_copy(step).wait_recv()

    def separate(shelf, put):
        for s in range(SLOT):
            for b in range(page_rows // block):
                split = jnp.dot(
                    perm[...],
                    pool_ref[shelf[s], b * block : (b + 1) * block, :],
                    preferred_element_type=jnp.float32,
                ).astype(jnp.bfloat16)
                for k in range(kv_count):
                    for kind in range(2):
                        low = (2 * k + kind) * block_tokens
                        put(k, s, kind, b * block_tokens, split[low : low + block_tokens])

    def send_pages(turn, carry):
        group = served(turn)
        await_tables(group)
        for step in range(1, inner):
            shelf, _, _ = request(group * inner + lax.rem(x + step, inner), me)

            def put(k, s, kind, at, rows_of):
                outgoing[step - 1, group, k, s, kind, at : at + block_tokens, :] = rows_of

            separate(shelf, put)
            for k in range(kv_count):
                page_copy(step, group, k).start()
        return carry

    lax.fori_loop(0, outer, send_pages, 0)

    for index in range(tiles):
        weight_copy(index).start()

    def list_pages(group, carry):
        for step in range(inner):
            shelf, dialog, fill = request(
                group * inner + x, z * inner + lax.rem(x - step + inner, inner)
            )
            for s in range(SLOT):
                listed[group, step, s, 0] = dialog[s]
                listed[group, step, s, 1] = fill[s]
            if step == 0:

                def put(k, s, kind, at, rows_of):
                    kept[group, k, s, kind, at : at + block_tokens, :] = rows_of

                separate(shelf, put)
        return carry

    lax.fori_loop(0, outer, list_pages, 0)

    fresh_rows = fresh_ref.shape[0]
    split = jnp.dot(
        selection(fresh_rows, kv_count), fresh_ref[...], preferred_element_type=jnp.float32
    ).astype(jnp.bfloat16)
    row_token = lax.broadcasted_iota(jnp.int32, (rows, token_rows), 0) % new_len
    col_token = lax.broadcasted_iota(jnp.int32, (rows, token_rows), 1)
    for k in range(kv_count):
        keys = split[(2 * k) * token_rows : (2 * k + 1) * token_rows]
        values = split[(2 * k + 1) * token_rows : (2 * k + 2) * token_rows]
        for d in range(dialogs):
            scores = lax.dot_general(
                qall[z, k, d], keys, CONTRACT, preferred_element_type=jnp.float32
            ) * scale
            causal = (col_token // new_len == d) & (col_token - d * new_len <= row_token)
            scores = jnp.where(causal, scores, floor_value)
            peak = jnp.max(scores, axis=-1, keepdims=True)
            weights = jnp.exp2(scores - peak).astype(jnp.bfloat16)
            peak_ref[z, k, d] = jnp.broadcast_to(peak, (rows, HD))
            amount_ref[z, k, d] = jnp.broadcast_to(
                jnp.sum(weights.astype(jnp.float32), axis=-1, keepdims=True), (rows, HD)
            )
            summed_ref[z, k, d] = jnp.dot(weights, values, preferred_element_type=jnp.float32)

    def absorb(group, k, step, pages, first):
        position = lax.broadcasted_iota(jnp.int32, (rows, PAGE), 1)
        dialog = [listed[group, step, s, 0] for s in range(SLOT)]
        fill = [listed[group, step, s, 1] for s in range(SLOT)]
        owned = [
            [jnp.broadcast_to(dialog[s], (rows, HD)) == d for d in range(dialogs)]
            for s in range(SLOT)
        ]
        for d in range(dialogs):
            qcur[d] = qall[group, k, d]
        scores, highs = [], []
        for s in range(SLOT):
            found = lax.dot_general(
                qcur[dialog[s]], pages[s, 0], CONTRACT, preferred_element_type=jnp.float32
            ) * scale
            found = jnp.where(position < fill[s], found, floor_value)
            scores.append(found)
            highs.append(jnp.broadcast_to(jnp.max(found, axis=-1, keepdims=True), (rows, HD)))
        peaks, keeps = [], []
        for d in range(dialogs):
            peak = functools.reduce(
                jnp.maximum,
                [jnp.where(owned[s][d], highs[s], floor_value) for s in range(SLOT)],
            )
            if not first:
                before = peak_ref[group, k, d]
                peak = jnp.maximum(peak, before)
                keeps.append(jnp.exp2(before - peak))
            peaks.append(peak)
            peak_ref[group, k, d] = peak
        amounts, sums = [], []
        for s in range(SLOT):
            peak = peaks[-1]
            for d in reversed(range(dialogs - 1)):
                peak = jnp.where(owned[s][d], peaks[d], peak)
            weights = jnp.exp2(scores[s] - peak).astype(jnp.bfloat16)
            amounts.append(
                jnp.broadcast_to(
                    jnp.sum(weights.astype(jnp.float32), axis=-1, keepdims=True), (rows, HD)
                )
            )
            sums.append(jnp.dot(weights, pages[s, 1], preferred_element_type=jnp.float32))
        for d in range(dialogs):
            amount = functools.reduce(
                jnp.add, [jnp.where(owned[s][d], amounts[s], 0.0) for s in range(SLOT)]
            )
            total = functools.reduce(
                jnp.add, [jnp.where(owned[s][d], sums[s], 0.0) for s in range(SLOT)]
            )
            if not first:
                amount = amount + keeps[d] * amount_ref[group, k, d]
                total = total + keeps[d] * summed_ref[group, k, d]
            amount_ref[group, k, d] = amount
            summed_ref[group, k, d] = total

    def absorb_kept(group, k, first):
        absorb(group, k, 0, kept.at[group, k], first)

    def absorb_arrived(group, k):
        for step in range(1, inner):
            page_copy(step, group, k).wait_recv()
            absorb(group, k, step, arrived.at[step - 1, group, k], False)

    def begin(k, carry):
        absorb_kept(z, k, False)
        return carry

    lax.fori_loop(0, kv_count, begin, 0)

    def relay(distance):
        for k in range(kv_count):
            @pl.when(z >= distance)
            def _():
                q_copy(z - distance, k, 0).wait_recv()

            @pl.when((z >= distance) & (z < outer - 1))
            def _():
                q_copy(z - distance, k, 0).start()

            @pl.when(z < outer - distance)
            def _():
                q_copy(z + distance, k, 1).wait_recv()

            @pl.when((z < outer - distance) & (z > 0))
            def _():
                q_copy(z + distance, k, 1).start()

    def serve(index, carry):
        group = served(index // kv_count)
        k = index % kv_count
        absorb_kept(group, k, True)
        absorb_arrived(group, k)
        for d in range(dialogs):
            amount = jnp.maximum(amount_ref[group, k, d], tiny_value)
            back[group, k, d] = (summed_ref[group, k, d] / amount).astype(jnp.bfloat16)
            log = peak_ref[group, k, d] + jnp.log2(amount)
            back_log[group, k, d : d + 1, :] = jnp.transpose(log)[:1]
        back_copy(group, k, z).start()
        log_copy(group, k, z).start()
        return carry

    for distance in range(1, half + 1):
        relay(distance)
    lax.fori_loop(0, kv_count, serve, 0)
    for distance in range(half + 1, outer):
        relay(distance)
    lax.fori_loop(kv_count, (outer - 1) * kv_count, serve, 0)

    def merge(turn, k):
        source = served(turn)
        back_copy(source, k, source).wait_recv()
        log_copy(source, k, source).wait_recv()
        for d in range(dialogs):
            line = came_log[source, k, d : d + 1, :]
            log = jnp.transpose(jnp.broadcast_to(line, (HD, rows)))
            before = peak_ref[z, k, d]
            peak = jnp.maximum(before, log)
            keep = jnp.exp2(before - peak)
            take = jnp.exp2(log - peak)
            peak_ref[z, k, d] = peak
            amount_ref[z, k, d] = keep * amount_ref[z, k, d] + take
            summed_ref[z, k, d] = keep * summed_ref[z, k, d] + take * came[
                source, k, d
            ].astype(jnp.float32)
        return k

    head_depth = per_group * HD

    def complete(k, carry):
        lax.fori_loop(0, half, merge, k)
        absorb_arrived(z, k)
        lax.fori_loop(half, outer - 1, merge, k)
        for d in range(dialogs):
            ratio = (summed_ref[z, k, d] / amount_ref[z, k, d]).astype(jnp.bfloat16)
            for g in range(per_group):
                attended[k, d * new_len : (d + 1) * new_len, g * HD : (g + 1) * HD] = ratio[
                    g * new_len : (g + 1) * new_len
                ]
        return carry

    def product_of(k, index):
        return jnp.dot(
            attended[k],
            wbuf[index, pl.ds(k * head_depth, head_depth), :],
            preferred_element_type=jnp.float32,
        )

    for k in range(kv_count):
        complete(k, 0)
        if k == kv_count - 1:
            break

        def collect(index, carry):
            if k == 0:
                weight_copy(index).wait()
                gathered[index] = product_of(k, index)
            else:
                gathered[index] += product_of(k, index)
            return carry

        lax.fori_loop(0, tiles, collect, 0)

    def join(index):
        core_copy(index).wait_recv()
        for step in range(1, chips):
            dest = lax.rem(chip + step, chips)
            total = part[index, core, dest].astype(jnp.float32) + sibling[index, dest].astype(
                jnp.float32
            )
            joined[index, step - 1] = total.astype(jnp.bfloat16)
            part_copy(index, step).start()

    def project(index, carry):
        if kv_count == 1:
            weight_copy(index).wait()
        product = product_of(kv_count - 1, index)
        if kv_count > 1:
            product = product + gathered[index]
        product = product.astype(jnp.bfloat16)
        for dest in range(shards):
            part[index, dest % CORES, dest // CORES] = product[
                dest * block_rows : (dest + 1) * block_rows
            ]
        core_copy(index).start()

        @pl.when(index >= LAG)
        def _():
            join(index - LAG)

        return carry

    lax.fori_loop(0, tiles, project, 0)

    def join_rest(index, carry):
        join(index)
        return carry

    lax.fori_loop(max(tiles - LAG, 0), tiles, join_rest, 0)

    def finish(index, carry):
        total = part[index, core, chip].astype(jnp.float32) + sibling[index, chip].astype(
            jnp.float32
        )
        for step in range(1, chips):
            part_copy(index, step).wait_recv()
            total = total + landed[index, step - 1].astype(jnp.float32)
        out_ref[:, pl.ds(pl.multiple_of(index * tile, tile), tile)] = total.astype(out_ref.dtype)
        return carry

    lax.fori_loop(0, tiles, finish, 0)

    def drain(index, carry):
        core_copy(index).wait_send()
        for step in range(1, chips):
            part_copy(index, step).wait_send()
        return carry

    lax.fori_loop(0, tiles, drain, 0)

    def drain_back(turn, carry):
        for k in range(kv_count):
            back_copy(served(turn), k, z).wait_send()
            log_copy(served(turn), k, z).wait_send()
        return carry

    lax.fori_loop(0, outer - 1, drain_back, 0)

    def drain_line(group, carry):
        for k in range(kv_count):
            for step in range(1, inner):
                page_copy(step, group, k).wait_send()

            @pl.when((group <= z) & (z < outer - 1))
            def _():
                q_copy(group, k, 0).wait_send()

            @pl.when((group >= z) & (z > 0))
            def _():
                q_copy(group, k, 1).wait_send()

        return carry

    lax.fori_loop(0, outer, drain_line, 0)
    for step in range(1, groups):
        table_copy(step).wait_send()
        length_copy(step).wait_send()


def local(queries, kv_new, pool, page_table, hist_len, o_weight):
    groups = lax.axis_size("replica")
    shards = lax.axis_size("tensor")
    outer, inner = spread(groups)
    pool_size, page_len, _, kv_width = pool.shape
    dialogs, entries = page_table.shape
    token_rows = queries.shape[0]
    new_len = token_rows // dialogs
    kv_count = kv_width // HD
    per_group = queries.shape[1] // kv_width
    rows = per_group * new_len
    depth, model = o_weight.shape
    tile = min(TILE, model)
    tiles = model // tile
    block_rows = token_rows // shards
    chips = shards // CORES
    page_rows = 2 * kv_count * page_len
    block = 256
    pages = pool.reshape(pool_size, page_len, 2, kv_count, HD).transpose(0, 1, 3, 2, 4)
    pages = pages.reshape(pool_size, page_rows, HD)
    fresh = kv_new.reshape(token_rows, 2, kv_count, HD).transpose(0, 2, 1, 3)
    fresh = fresh.reshape(2 * kv_count * token_rows, HD)
    vmem = pl.BlockSpec(memory_space=pltpu.VMEM)
    anywhere = pl.BlockSpec(memory_space=pl.ANY)
    dma = pltpu.SemaphoreType.DMA
    bf16, f32 = jnp.bfloat16, jnp.float32
    return pl.pallas_call(
        functools.partial(kernel, groups, shards),
        out_shape=jax.ShapeDtypeStruct((block_rows, model), jnp.bfloat16),
        in_specs=[anywhere] * 6,
        out_specs=vmem,
        scratch_shapes=[
            pltpu.SMEM((groups, dialogs, entries), jnp.int32),
            pltpu.SMEM((groups, dialogs), jnp.int32),
            pltpu.SMEM((outer, inner, SLOT, 2), jnp.int32),
            pltpu.VMEM((pool_size, page_rows, HD), bf16),
            pltpu.VMEM((2 * kv_count * token_rows, HD), bf16),
            pltpu.VMEM((outer, kv_count, SLOT, 2, page_len, HD), bf16),
            pltpu.VMEM((inner - 1, outer, kv_count, SLOT, 2, page_len, HD), bf16),
            pltpu.VMEM((inner - 1, outer, kv_count, SLOT, 2, page_len, HD), bf16),
            pltpu.VMEM((tiles, depth, tile), bf16),
            pltpu.VMEM((block, block), bf16),
            pltpu.VMEM((outer, kv_count, dialogs, rows, HD), bf16),
            pltpu.VMEM((dialogs, rows, HD), bf16),
            pltpu.VMEM((outer, kv_count, dialogs, rows, HD), f32),
            pltpu.VMEM((outer, kv_count, dialogs, rows, HD), f32),
            pltpu.VMEM((outer, kv_count, dialogs, rows, HD), f32),
            pltpu.VMEM((outer, kv_count, dialogs, rows, HD), bf16),
            pltpu.VMEM((outer, kv_count, dialogs, rows), f32),
            pltpu.VMEM((outer, kv_count, dialogs, rows, HD), bf16),
            pltpu.VMEM((outer, kv_count, dialogs, rows), f32),
            pltpu.VMEM((kv_count, token_rows, depth // kv_count), bf16),
            pltpu.VMEM((tiles, token_rows, tile), f32),
            pltpu.VMEM((tiles, CORES, chips, block_rows, tile), bf16),
            pltpu.VMEM((tiles, chips, block_rows, tile), bf16),
            pltpu.VMEM((tiles, chips - 1, block_rows, tile), bf16),
            pltpu.VMEM((tiles, chips - 1, block_rows, tile), bf16),
            dma((4,)),
            dma((kv_count, dialogs, per_group)),
            dma((tiles,)),
            dma((groups,)),
            dma((groups,)),
            dma((groups,)),
            dma((groups,)),
            dma((2, outer, kv_count)),
            dma((outer, kv_count)),
            dma((inner - 1, outer, kv_count)),
            dma((inner - 1, outer, kv_count)),
            dma((outer, kv_count)),
            dma((outer, kv_count)),
            dma((outer, kv_count)),
            dma((outer, kv_count)),
            dma((tiles,)),
            dma((tiles,)),
            dma((tiles, chips - 1)),
            dma((tiles, chips - 1)),
        ],
        compiler_params=pltpu.CompilerParams(
            collective_id=0, has_side_effects=True, vmem_limit_bytes=63 * 1024 * 1024
        ),
        name="attend",
    )(queries, fresh, pages, page_table, hist_len, o_weight)


def solution(mesh):
    in_specs = (
        P("replica", "tensor"),
        P("replica", None, "tensor"),
        P("replica", None, None, "tensor"),
        P("replica", None),
        P("replica"),
        P("tensor", None),
    )
    out_specs = P(("replica", "tensor"), None)
    return jax.shard_map(local, mesh=mesh, in_specs=in_specs, out_specs=out_specs, check_vma=False)
```

```python
import functools
import math

import jax
import jax.numpy as jnp
from jax import lax
from jax.experimental import pallas as pl
from jax.experimental.pallas import tpu as pltpu
from jax.sharding import PartitionSpec as P

HD = 128
PAGE = 128
SLOT = 3
TILE = 1024
LAG = 2
CORES = 2

floor_value = -1e30
tiny_value = 1e-30

MESH = pl.DeviceIdType.MESH
CONTRACT = (((1,), (1,)), ((), ()))


def spread(groups):
    outer = 1
    while outer * outer < groups:
        outer *= 2
    return outer, groups // outer


def selection(rows, kv_count):
    kinds = 2 * kv_count
    tokens = rows // kinds
    i = lax.broadcasted_iota(jnp.int32, (rows, rows), 0)
    j = lax.broadcasted_iota(jnp.int32, (rows, rows), 1)
    source = (i % tokens) * kinds + i // tokens
    return jnp.where(source == j, 1.0, 0.0).astype(jnp.bfloat16)


def kernel(
    groups, shards,
    q_hbm, fresh_hbm, pool_hbm, table_hbm, length_hbm, weight,
    out_ref,
    table, length, listed, pool_ref, fresh_ref, kept, kept_side, outgoing, arrived, wbuf, perm,
    qall, qside, qcur,
    peak_ref, amount_ref, summed_ref, back, back_log, came, came_log, attended, gathered,
    part, sibling, joined, landed,
    load_sem, q_load_sem, weight_sem,
    row_send, row_recv, line_send, line_recv,
    q_send, q_recv, side_send, side_recv, page_send, page_recv,
    back_send, back_recv, log_send, log_recv,
    core_send, core_recv, part_send, part_recv,
):
    outer, inner = spread(groups)
    half = outer // 2
    me = lax.axis_index("replica")
    mine = lax.axis_index("tensor")
    z = me // inner
    x = me % inner
    pool_size = pool_ref.shape[0]
    _, kv_count, dialogs, rows, _ = qall.shape
    entries = table.shape[3]
    token_rows = q_hbm.shape[0]
    new_len = token_rows // dialogs
    per_group = rows // new_len
    tiles, _, chips, block_rows, tile = part.shape
    block = perm.shape[0]
    page_rows = pool_ref.shape[1]
    block_tokens = block // (2 * kv_count)
    scale = math.log2(math.e) / math.sqrt(HD)
    chip = mine // CORES
    core = mine % CORES

    loads = [
        pltpu.make_async_copy(table_hbm, table.at[z, x], load_sem.at[0]),
        pltpu.make_async_copy(length_hbm, length.at[z, x], load_sem.at[1]),
        pltpu.make_async_copy(pool_hbm, pool_ref, load_sem.at[2]),
        pltpu.make_async_copy(fresh_hbm, fresh_ref, load_sem.at[3]),
    ]

    def q_load(k, d, g):
        col = (k * per_group + g) * HD
        return pltpu.make_async_copy(
            q_hbm.at[d * new_len : (d + 1) * new_len, col : col + HD],
            qall.at[z, k, d, g * new_len : (g + 1) * new_len, :],
            q_load_sem.at[k, d, g],
        )

    q_loads = [
        q_load(k, d, g) for k in range(kv_count) for d in range(dialogs) for g in range(per_group)
    ]

    loads[0].start()
    loads[1].start()
    for copy in q_loads:
        copy.start()
    loads[2].start()
    loads[3].start()

    barrier = pltpu.get_barrier_semaphore()
    for step in range(1, inner):
        pl.semaphore_signal(
            barrier,
            inc=1,
            device_id={"replica": z * inner + lax.rem(x + step, inner)},
            device_id_type=MESH,
        )

    @pl.when(z < outer - 1)
    def _():
        pl.semaphore_signal(
            barrier, inc=1, device_id={"replica": me + inner}, device_id_type=MESH
        )

    @pl.when(z > 0)
    def _():
        pl.semaphore_signal(
            barrier, inc=1, device_id={"replica": me - inner}, device_id_type=MESH
        )

    for step in range(1, shards):
        pl.semaphore_signal(
            barrier, inc=1, device_id={"tensor": lax.rem(mine + step, shards)}, device_id_type=MESH
        )

    def row_copies(step):
        return [
            pltpu.make_async_remote_copy(
                src_ref=ref.at[z, x],
                dst_ref=ref.at[z, x],
                send_sem=row_send.at[which, step - 1],
                recv_sem=row_recv.at[which, step - 1],
                device_id={"replica": z * inner + lax.rem(x + step, inner)},
                device_id_type=MESH,
            )
            for which, ref in enumerate((table, length))
        ]

    def line_copies(group, way):
        dest = z + (1 if way == 0 else -1)
        return [
            pltpu.make_async_remote_copy(
                src_ref=ref.at[group],
                dst_ref=ref.at[group],
                send_sem=line_send.at[which, way, group],
                recv_sem=line_recv.at[which, group],
                device_id={"replica": dest * inner + x},
                device_id_type=MESH,
            )
            for which, ref in enumerate((table, length))
        ]

    def start(copies):
        for copy in copies:
            copy.start()

    def wait_recv(copies):
        for copy in copies:
            copy.wait_recv()

    def side_q_copy(step, k):
        return pltpu.make_async_remote_copy(
            src_ref=qall.at[z, k],
            dst_ref=qside.at[step - 1, k],
            send_sem=side_send.at[step - 1, k],
            recv_sem=side_recv.at[step - 1, k],
            device_id={"replica": z * inner + lax.rem(x + step, inner)},
            device_id_type=MESH,
        )

    def q_copy(group, k, way):
        dest = z + (1 if way == 0 else -1)
        return pltpu.make_async_remote_copy(
            src_ref=qall.at[group, k],
            dst_ref=qall.at[group, k],
            send_sem=q_send.at[way, group, k],
            recv_sem=q_recv.at[group, k],
            device_id={"replica": dest * inner + x},
            device_id_type=MESH,
        )

    def page_copy(step, group, k):
        return pltpu.make_async_remote_copy(
            src_ref=outgoing.at[step - 1, group, k],
            dst_ref=arrived.at[step - 1, group, k],
            send_sem=page_send.at[step - 1, group, k],
            recv_sem=page_recv.at[step - 1, group, k],
            device_id={"replica": z * inner + lax.rem(x + step, inner)},
            device_id_type=MESH,
        )

    def back_copy(group, k, source):
        return pltpu.make_async_remote_copy(
            src_ref=back.at[group, k],
            dst_ref=came.at[source, k],
            send_sem=back_send.at[group, k],
            recv_sem=back_recv.at[source, k],
            device_id={"replica": group * inner + x},
            device_id_type=MESH,
        )

    def log_copy(group, k, source):
        return pltpu.make_async_remote_copy(
            src_ref=back_log.at[group, k],
            dst_ref=came_log.at[source, k],
            send_sem=log_send.at[group, k],
            recv_sem=log_recv.at[source, k],
            device_id={"replica": group * inner + x},
            device_id_type=MESH,
        )

    def side_copies(step, k):
        return [
            pltpu.make_async_remote_copy(
                src_ref=src.at[outer + step - 1, k],
                dst_ref=dst.at[outer + step - 1, k],
                send_sem=sends.at[outer + step - 1, k],
                recv_sem=recvs.at[outer + step - 1, k],
                device_id={"replica": z * inner + lax.rem(x - step + inner, inner)},
                device_id_type=MESH,
            )
            for src, dst, sends, recvs in (
                (back, came, back_send, back_recv),
                (back_log, came_log, log_send, log_recv),
            )
        ]

    def weight_copy(index):
        return pltpu.make_async_copy(
            weight.at[:, pl.ds(pl.multiple_of(index * tile, tile), tile)],
            wbuf.at[index],
            weight_sem.at[index],
        )

    def core_copy(index):
        return pltpu.make_async_remote_copy(
            src_ref=part.at[index, 1 - core],
            dst_ref=sibling.at[index],
            send_sem=core_send.at[index],
            recv_sem=core_recv.at[index],
            device_id={"tensor": chip * CORES + 1 - core},
            device_id_type=MESH,
        )

    def part_copy(index, step):
        dest = lax.rem(chip + step, chips)
        return pltpu.make_async_remote_copy(
            src_ref=joined.at[index, step - 1],
            dst_ref=landed.at[index, step - 1],
            send_sem=part_send.at[index, step - 1],
            recv_sem=part_recv.at[index, step - 1],
            device_id={"tensor": dest * CORES + core},
            device_id_type=MESH,
        )

    perm[...] = selection(block, kv_count)

    side = z // half

    def served(turn):
        across = (1 - side) * (half + turn) + side * (half - 1 - turn)
        beside = side * half + lax.rem(z - side * half + 1 + turn - half + outer, half)
        far = (turn < half).astype(jnp.int32) if not isinstance(turn, int) else int(turn < half)
        return far * across + (1 - far) * beside

    loads[0].wait()
    loads[1].wait()
    beside_line = (z > 0).astype(jnp.int32) + (z < outer - 1).astype(jnp.int32)
    pl.semaphore_wait(barrier, inner - 1 + shards - 1 + beside_line)
    for step in range(1, inner):
        start(row_copies(step))
    for copy in q_loads:
        copy.wait()
    for k in range(kv_count):
        @pl.when(z < outer - 1)
        def _():
            q_copy(z, k, 0).start()

        @pl.when(z > 0)
        def _():
            q_copy(z, k, 1).start()

        for step in range(1, inner):
            side_q_copy(step, k).start()

    for step in range(1, inner):
        wait_recv(row_copies(step))

    @pl.when(z < outer - 1)
    def _():
        start(line_copies(z, 0))

    @pl.when(z > 0)
    def _():
        start(line_copies(z, 1))

    loads[2].wait()
    loads[3].wait()

    def request(group, owner):
        count = jnp.int32(0)
        zero = jnp.int32(0)
        shelf, dialog, fill = [zero] * SLOT, [zero] * SLOT, [zero] * SLOT
        low = owner * pool_size
        for d in range(dialogs):
            total = length[group // inner, group % inner, d]
            for e in range(entries):
                place = table[group // inner, group % inner, d, e] - low
                live = jnp.minimum(total - e * PAGE, PAGE)
                hit = (place >= 0) & (place < pool_size) & (live > 0)
                for s in range(SLOT):
                    here = hit & (count == s)
                    shelf[s] = jnp.where(here, place, shelf[s])
                    dialog[s] = jnp.where(here, d, dialog[s])
                    fill[s] = jnp.where(here, live, fill[s])
                count = count + hit.astype(jnp.int32)
        return shelf, dialog, fill

    def relay_tables(distance):
        @pl.when(z >= distance)
        def _():
            wait_recv(line_copies(z - distance, 0))

        @pl.when((z >= distance) & (z < outer - 1))
        def _():
            start(line_copies(z - distance, 0))

        @pl.when(z < outer - distance)
        def _():
            wait_recv(line_copies(z + distance, 1))

        @pl.when((z < outer - distance) & (z > 0))
        def _():
            start(line_copies(z + distance, 1))

    def separate(shelf, put):
        for s in range(SLOT):
            for b in range(page_rows // block):
                split = jnp.dot(
                    perm[...],
                    pool_ref[shelf[s], b * block : (b + 1) * block, :],
                    preferred_element_type=jnp.float32,
                ).astype(jnp.bfloat16)
                for k in range(kv_count):
                    for kind in range(2):
                        low = (2 * k + kind) * block_tokens
                        put(k, s, kind, b * block_tokens, split[low : low + block_tokens])

    def relay(distance, k):
        @pl.when(z >= distance)
        def _():
            q_copy(z - distance, k, 0).wait_recv()

        @pl.when((z >= distance) & (z < outer - 1))
        def _():
            q_copy(z - distance, k, 0).start()

        @pl.when(z < outer - distance)
        def _():
            q_copy(z + distance, k, 1).wait_recv()

        @pl.when((z < outer - distance) & (z > 0))
        def _():
            q_copy(z + distance, k, 1).start()

    def send_pages(turn, carry):
        group = served(turn)
        for step in range(1, inner):
            shelf, _, _ = request(group * inner + lax.rem(x + step, inner), me)

            def put(k, s, kind, at, rows_of):
                outgoing[step - 1, group, k, s, kind, at : at + block_tokens, :] = rows_of

            separate(shelf, put)
            for k in range(kv_count):
                page_copy(step, group, k).start()
        return carry

    for distance in range(1, half + 1):
        relay_tables(distance)
        if distance < half:
            relay(distance, 0)
    lax.fori_loop(0, 1, send_pages, 0)
    for k in range(1, kv_count):
        for distance in range(1, half):
            relay(distance, k)
    for distance in range(half + 1, outer):
        relay_tables(distance)
    lax.fori_loop(1, outer - 1, send_pages, 0)

    for index in range(tiles):
        weight_copy(index).start()

    def list_pages(group, carry):
        for step in range(inner):
            behind = lax.rem(x - step + inner, inner)
            own_row = (group == z).astype(jnp.int32)
            shelf, dialog, fill = request(
                group * inner + own_row * behind + (1 - own_row) * x,
                z * inner + own_row * x + (1 - own_row) * behind,
            )
            for s in range(SLOT):
                listed[group, step, s, 0] = dialog[s]
                listed[group, step, s, 1] = fill[s]
                listed[group, step, s, 2] = shelf[s]
            if step == 0:

                def put(k, s, kind, at, rows_of):
                    kept[group, k, s, kind, at : at + block_tokens, :] = rows_of

                separate(shelf, put)
        return carry

    lax.fori_loop(0, half, list_pages, 0)
    relay(half, 0)
    lax.fori_loop(half, outer, list_pages, 0)
    for step in range(1, inner):

        def put_side(k, s, kind, at, rows_of):
            kept_side[step - 1, k, s, kind, at : at + block_tokens, :] = rows_of

        separate([listed[z, step, s, 2] for s in range(SLOT)], put_side)

    fresh_rows = fresh_ref.shape[0]
    split = jnp.dot(
        selection(fresh_rows, kv_count), fresh_ref[...], preferred_element_type=jnp.float32
    ).astype(jnp.bfloat16)
    row_token = lax.broadcasted_iota(jnp.int32, (rows, token_rows), 0) % new_len
    col_token = lax.broadcasted_iota(jnp.int32, (rows, token_rows), 1)
    for k in range(kv_count):
        keys = split[(2 * k) * token_rows : (2 * k + 1) * token_rows]
        values = split[(2 * k + 1) * token_rows : (2 * k + 2) * token_rows]
        for d in range(dialogs):
            scores = lax.dot_general(
                qall[z, k, d], keys, CONTRACT, preferred_element_type=jnp.float32
            ) * scale
            causal = (col_token // new_len == d) & (col_token - d * new_len <= row_token)
            scores = jnp.where(causal, scores, floor_value)
            peak = jnp.max(scores, axis=-1, keepdims=True)
            weights = jnp.exp2(scores - peak).astype(jnp.bfloat16)
            peak_ref[z, k, d] = jnp.broadcast_to(peak, (rows, HD))
            amount_ref[z, k, d] = jnp.broadcast_to(
                jnp.sum(weights.astype(jnp.float32), axis=-1, keepdims=True), (rows, HD)
            )
            summed_ref[z, k, d] = jnp.dot(weights, values, preferred_element_type=jnp.float32)

    for k in range(1, kv_count):
        relay(half, k)

    def absorb(group, k, q_ref, listing, pages, first):
        position = lax.broadcasted_iota(jnp.int32, (rows, PAGE), 1)
        dialog = [listing[s, 0] for s in range(SLOT)]
        fill = [listing[s, 1] for s in range(SLOT)]
        owned = [
            [jnp.broadcast_to(dialog[s], (rows, HD)) == d for d in range(dialogs)]
            for s in range(SLOT)
        ]
        for d in range(dialogs):
            qcur[d] = q_ref[k, d]
        scores, highs = [], []
        for s in range(SLOT):
            found = lax.dot_general(
                qcur[dialog[s]], pages[s, 0], CONTRACT, preferred_element_type=jnp.float32
            ) * scale
            found = jnp.where(position < fill[s], found, floor_value)
            scores.append(found)
            highs.append(jnp.broadcast_to(jnp.max(found, axis=-1, keepdims=True), (rows, HD)))
        peaks, keeps = [], []
        for d in range(dialogs):
            peak = functools.reduce(
                jnp.maximum,
                [jnp.where(owned[s][d], highs[s], floor_value) for s in range(SLOT)],
            )
            if not first:
                before = peak_ref[group, k, d]
                peak = jnp.maximum(peak, before)
                keeps.append(jnp.exp2(before - peak))
            peaks.append(peak)
            peak_ref[group, k, d] = peak
        amounts, sums = [], []
        for s in range(SLOT):
            peak = peaks[-1]
            for d in reversed(range(dialogs - 1)):
                peak = jnp.where(owned[s][d], peaks[d], peak)
            weights = jnp.exp2(scores[s] - peak).astype(jnp.bfloat16)
            amounts.append(
                jnp.broadcast_to(
                    jnp.sum(weights.astype(jnp.float32), axis=-1, keepdims=True), (rows, HD)
                )
            )
            sums.append(jnp.dot(weights, pages[s, 1], preferred_element_type=jnp.float32))
        for d in range(dialogs):
            amount = functools.reduce(
                jnp.add, [jnp.where(owned[s][d], amounts[s], 0.0) for s in range(SLOT)]
            )
            total = functools.reduce(
                jnp.add, [jnp.where(owned[s][d], sums[s], 0.0) for s in range(SLOT)]
            )
            if not first:
                amount = amount + keeps[d] * amount_ref[group, k, d]
                total = total + keeps[d] * summed_ref[group, k, d]
            amount_ref[group, k, d] = amount
            summed_ref[group, k, d] = total

    def absorb_kept(group, k, first):
        absorb(group, k, qall.at[group], listed.at[group, 0], kept.at[group, k], first)

    def absorb_arrived(group, k):
        for step in range(1, inner):
            page_copy(step, group, k).wait_recv()
            absorb(
                group,
                k,
                qall.at[group],
                listed.at[group, step],
                arrived.at[step - 1, group, k],
                False,
            )

    def begin(k, carry):
        absorb_kept(z, k, False)
        return carry

    lax.fori_loop(0, kv_count, begin, 0)

    def pack(slot, k):
        for d in range(dialogs):
            amount = jnp.maximum(amount_ref[slot, k, d], tiny_value)
            back[slot, k, d] = (summed_ref[slot, k, d] / amount).astype(jnp.bfloat16)
            log = peak_ref[slot, k, d] + jnp.log2(amount)
            back_log[slot, k, d : d + 1, :] = jnp.transpose(log)[:1]

    def serve(index, carry):
        group = served(index // kv_count)
        k = index % kv_count
        absorb_kept(group, k, True)
        absorb_arrived(group, k)
        pack(group, k)
        back_copy(group, k, z).start()
        log_copy(group, k, z).start()
        return carry

    def serve_then_relay(index, carry):
        serve(index, 0)
        relay(half + 1 + index // kv_count, index % kv_count)
        return carry

    def serve_row(k, carry):
        for step in range(1, inner):
            side_q_copy(step, k).wait_recv()
            slot = outer + step - 1
            absorb(
                slot,
                k,
                qside.at[step - 1],
                listed.at[z, step],
                kept_side.at[step - 1, k],
                True,
            )
            pack(slot, k)
            start(side_copies(step, k))
        return carry

    lax.fori_loop(0, kv_count, serve_then_relay, 0)
    lax.fori_loop(0, kv_count, serve_row, 0)
    lax.fori_loop(kv_count, (half - 1) * kv_count, serve_then_relay, 0)
    lax.fori_loop((half - 1) * kv_count, (outer - 1) * kv_count, serve, 0)

    def merge(turn, k):
        source = served(turn)
        back_copy(source, k, source).wait_recv()
        log_copy(source, k, source).wait_recv()
        merge_slot(source, k)
        return k

    def merge_slot(source, k):
        for d in range(dialogs):
            line = came_log[source, k, d : d + 1, :]
            log = jnp.transpose(jnp.broadcast_to(line, (HD, rows)))
            before = peak_ref[z, k, d]
            peak = jnp.maximum(before, log)
            keep = jnp.exp2(before - peak)
            take = jnp.exp2(log - peak)
            peak_ref[z, k, d] = peak
            amount_ref[z, k, d] = keep * amount_ref[z, k, d] + take
            summed_ref[z, k, d] = keep * summed_ref[z, k, d] + take * came[
                source, k, d
            ].astype(jnp.float32)

    head_depth = per_group * HD

    def complete(k, carry):
        lax.fori_loop(0, half, merge, k)
        lax.fori_loop(half, outer - 1, merge, k)
        for step in range(1, inner):
            wait_recv(side_copies(step, k))
            merge_slot(outer + step - 1, k)
        for d in range(dialogs):
            ratio = (summed_ref[z, k, d] / amount_ref[z, k, d]).astype(jnp.bfloat16)
            for g in range(per_group):
                attended[k, d * new_len : (d + 1) * new_len, g * HD : (g + 1) * HD] = ratio[
                    g * new_len : (g + 1) * new_len
                ]
        return carry

    def product_of(k, index):
        return jnp.dot(
            attended[k],
            wbuf[index, pl.ds(k * head_depth, head_depth), :],
            preferred_element_type=jnp.float32,
        )

    for k in range(kv_count):
        complete(k, 0)
        if k == kv_count - 1:
            break

        def collect(index, carry):
            if k == 0:
                weight_copy(index).wait()
                gathered[index] = product_of(k, index)
            else:
                gathered[index] += product_of(k, index)
            return carry

        lax.fori_loop(0, tiles, collect, 0)

    def join(index):
        core_copy(index).wait_recv()
        for step in range(1, chips):
            dest = lax.rem(chip + step, chips)
            total = part[index, core, dest].astype(jnp.float32) + sibling[index, dest].astype(
                jnp.float32
            )
            joined[index, step - 1] = total.astype(jnp.bfloat16)
            part_copy(index, step).start()

    def project(index, carry):
        if kv_count == 1:
            weight_copy(index).wait()
        product = product_of(kv_count - 1, index)
        if kv_count > 1:
            product = product + gathered[index]
        product = product.astype(jnp.bfloat16)
        for dest in range(shards):
            part[index, dest % CORES, dest // CORES] = product[
                dest * block_rows : (dest + 1) * block_rows
            ]
        core_copy(index).start()

        @pl.when(index >= LAG)
        def _():
            join(index - LAG)

        return carry

    lax.fori_loop(0, tiles, project, 0)

    def join_rest(index, carry):
        join(index)
        return carry

    lax.fori_loop(max(tiles - LAG, 0), tiles, join_rest, 0)

    def finish(index, carry):
        total = part[index, core, chip].astype(jnp.float32) + sibling[index, chip].astype(
            jnp.float32
        )
        for step in range(1, chips):
            part_copy(index, step).wait_recv()
            total = total + landed[index, step - 1].astype(jnp.float32)
        out_ref[:, pl.ds(pl.multiple_of(index * tile, tile), tile)] = total.astype(out_ref.dtype)
        return carry

    lax.fori_loop(0, tiles, finish, 0)

    def drain(index, carry):
        core_copy(index).wait_send()
        for step in range(1, chips):
            part_copy(index, step).wait_send()
        return carry

    lax.fori_loop(0, tiles, drain, 0)

    def drain_back(turn, carry):
        for k in range(kv_count):
            back_copy(served(turn), k, z).wait_send()
            log_copy(served(turn), k, z).wait_send()
        return carry

    lax.fori_loop(0, outer - 1, drain_back, 0)

    def drain_line(group, carry):
        for k in range(kv_count):
            @pl.when((group <= z) & (z < outer - 1))
            def _():
                q_copy(group, k, 0).wait_send()

            @pl.when((group >= z) & (z > 0))
            def _():
                q_copy(group, k, 1).wait_send()

            @pl.when(group != z)
            def _():
                for step in range(1, inner):
                    page_copy(step, group, k).wait_send()

        @pl.when((group <= z) & (z < outer - 1))
        def _():
            for copy in line_copies(group, 0):
                copy.wait_send()

        @pl.when((group >= z) & (z > 0))
        def _():
            for copy in line_copies(group, 1):
                copy.wait_send()

        return carry

    lax.fori_loop(0, outer, drain_line, 0)
    for step in range(1, inner):
        for copy in row_copies(step):
            copy.wait_send()
        for k in range(kv_count):
            side_q_copy(step, k).wait_send()
            for copy in side_copies(step, k):
                copy.wait_send()


def local(queries, kv_new, pool, page_table, hist_len, o_weight):
    groups = lax.axis_size("replica")
    shards = lax.axis_size("tensor")
    outer, inner = spread(groups)
    pool_size, page_len, _, kv_width = pool.shape
    dialogs, entries = page_table.shape
    token_rows = queries.shape[0]
    new_len = token_rows // dialogs
    kv_count = kv_width // HD
    per_group = queries.shape[1] // kv_width
    rows = per_group * new_len
    depth, model = o_weight.shape
    tile = min(TILE, model)
    tiles = model // tile
    block_rows = token_rows // shards
    chips = shards // CORES
    page_rows = 2 * kv_count * page_len
    slots = outer + inner - 1
    block = 256
    pages = pool.reshape(pool_size, page_len, 2, kv_count, HD).transpose(0, 1, 3, 2, 4)
    pages = pages.reshape(pool_size, page_rows, HD)
    fresh = kv_new.reshape(token_rows, 2, kv_count, HD).transpose(0, 2, 1, 3)
    fresh = fresh.reshape(2 * kv_count * token_rows, HD)
    vmem = pl.BlockSpec(memory_space=pltpu.VMEM)
    anywhere = pl.BlockSpec(memory_space=pl.ANY)
    dma = pltpu.SemaphoreType.DMA
    bf16, f32 = jnp.bfloat16, jnp.float32
    return pl.pallas_call(
        functools.partial(kernel, groups, shards),
        out_shape=jax.ShapeDtypeStruct((block_rows, model), jnp.bfloat16),
        in_specs=[anywhere] * 6,
        out_specs=vmem,
        scratch_shapes=[
            pltpu.SMEM((outer, inner, dialogs, entries), jnp.int32),
            pltpu.SMEM((outer, inner, dialogs), jnp.int32),
            pltpu.SMEM((outer, inner, SLOT, 3), jnp.int32),
            pltpu.VMEM((pool_size, page_rows, HD), bf16),
            pltpu.VMEM((2 * kv_count * token_rows, HD), bf16),
            pltpu.VMEM((outer, kv_count, SLOT, 2, page_len, HD), bf16),
            pltpu.VMEM((inner - 1, kv_count, SLOT, 2, page_len, HD), bf16),
            pltpu.VMEM((inner - 1, outer, kv_count, SLOT, 2, page_len, HD), bf16),
            pltpu.VMEM((inner - 1, outer, kv_count, SLOT, 2, page_len, HD), bf16),
            pltpu.VMEM((tiles, depth, tile), bf16),
            pltpu.VMEM((block, block), bf16),
            pltpu.VMEM((outer, kv_count, dialogs, rows, HD), bf16),
            pltpu.VMEM((inner - 1, kv_count, dialogs, rows, HD), bf16),
            pltpu.VMEM((dialogs, rows, HD), bf16),
            pltpu.VMEM((slots, kv_count, dialogs, rows, HD), f32),
            pltpu.VMEM((slots, kv_count, dialogs, rows, HD), f32),
            pltpu.VMEM((slots, kv_count, dialogs, rows, HD), f32),
            pltpu.VMEM((slots, kv_count, dialogs, rows, HD), bf16),
            pltpu.VMEM((slots, kv_count, dialogs, rows), f32),
            pltpu.VMEM((slots, kv_count, dialogs, rows, HD), bf16),
            pltpu.VMEM((slots, kv_count, dialogs, rows), f32),
            pltpu.VMEM((kv_count, token_rows, depth // kv_count), bf16),
            pltpu.VMEM((tiles, token_rows, tile), f32),
            pltpu.VMEM((tiles, CORES, chips, block_rows, tile), bf16),
            pltpu.VMEM((tiles, chips, block_rows, tile), bf16),
            pltpu.VMEM((tiles, chips - 1, block_rows, tile), bf16),
            pltpu.VMEM((tiles, chips - 1, block_rows, tile), bf16),
            dma((4,)),
            dma((kv_count, dialogs, per_group)),
            dma((tiles,)),
            dma((2, inner - 1)),
            dma((2, inner - 1)),
            dma((2, 2, outer)),
            dma((2, outer)),
            dma((2, outer, kv_count)),
            dma((outer, kv_count)),
            dma((inner - 1, kv_count)),
            dma((inner - 1, kv_count)),
            dma((inner - 1, outer, kv_count)),
            dma((inner - 1, outer, kv_count)),
            dma((slots, kv_count)),
            dma((slots, kv_count)),
            dma((slots, kv_count)),
            dma((slots, kv_count)),
            dma((tiles,)),
            dma((tiles,)),
            dma((tiles, chips - 1)),
            dma((tiles, chips - 1)),
        ],
        compiler_params=pltpu.CompilerParams(
            collective_id=0, has_side_effects=True, vmem_limit_bytes=63 * 1024 * 1024
        ),
        name="attend",
    )(queries, fresh, pages, page_table, hist_len, o_weight)


def solution(mesh):
    in_specs = (
        P("replica", "tensor"),
        P("replica", None, "tensor"),
        P("replica", None, None, "tensor"),
        P("replica", None),
        P("replica"),
        P("tensor", None),
    )
    out_specs = P(("replica", "tensor"), None)
    return jax.shard_map(local, mesh=mesh, in_specs=in_specs, out_specs=out_specs, check_vma=False)
```

```python
import functools
import math

import jax
import jax.numpy as jnp
from jax import lax
from jax.experimental import pallas as pl
from jax.experimental.pallas import tpu as pltpu
from jax.sharding import PartitionSpec as P

HD = 128
PAGE = 128
SLOT = 3
TILE = 1024
LAG = 2
CORES = 2

floor_value = -1e30
tiny_value = 1e-30

MESH = pl.DeviceIdType.MESH
CONTRACT = (((1,), (1,)), ((), ()))


def spread(groups):
    outer = 1
    while outer * outer < groups:
        outer *= 2
    return outer, groups // outer


def selection(rows, kv_count):
    kinds = 2 * kv_count
    tokens = rows // kinds
    i = lax.broadcasted_iota(jnp.int32, (rows, rows), 0)
    j = lax.broadcasted_iota(jnp.int32, (rows, rows), 1)
    source = (i % tokens) * kinds + i // tokens
    return jnp.where(source == j, 1.0, 0.0).astype(jnp.bfloat16)


def kernel(
    groups, shards,
    q_hbm, fresh_hbm, pool_hbm, table_hbm, length_hbm, weight,
    out_ref,
    table, length, listed, pool_ref, fresh_ref, kept, outgoing, arrived, wbuf, perm, qall, qcur,
    peak_ref, amount_ref, summed_ref, back, back_log, came, came_log, attended, gathered,
    part, sibling, joined, landed,
    load_sem, q_load_sem, weight_sem,
    table_send, table_recv, length_send, length_recv,
    q_send, q_recv, page_send, page_recv,
    back_send, back_recv, log_send, log_recv,
    core_send, core_recv, part_send, part_recv,
):
    outer, inner = spread(groups)
    half = outer // 2
    me = lax.axis_index("replica")
    mine = lax.axis_index("tensor")
    z = me // inner
    x = me % inner
    pool_size = pool_ref.shape[0]
    _, kv_count, dialogs, rows, _ = qall.shape
    entries = table.shape[2]
    token_rows = q_hbm.shape[0]
    new_len = token_rows // dialogs
    per_group = rows // new_len
    tiles, _, chips, block_rows, tile = part.shape
    block = perm.shape[0]
    page_rows = pool_ref.shape[1]
    block_tokens = block // (2 * kv_count)
    scale = math.log2(math.e) / math.sqrt(HD)
    chip = mine // CORES
    core = mine % CORES

    loads = [
        pltpu.make_async_copy(table_hbm, table.at[me], load_sem.at[0]),
        pltpu.make_async_copy(length_hbm, length.at[me], load_sem.at[1]),
        pltpu.make_async_copy(pool_hbm, pool_ref, load_sem.at[2]),
        pltpu.make_async_copy(fresh_hbm, fresh_ref, load_sem.at[3]),
    ]

    def q_load(k, d, g):
        col = (k * per_group + g) * HD
        return pltpu.make_async_copy(
            q_hbm.at[d * new_len : (d + 1) * new_len, col : col + HD],
            qall.at[z, k, d, g * new_len : (g + 1) * new_len, :],
            q_load_sem.at[k, d, g],
        )

    q_loads = [
        q_load(k, d, g) for k in range(kv_count) for d in range(dialogs) for g in range(per_group)
    ]

    loads[0].start()
    loads[1].start()
    for copy in q_loads:
        copy.start()
    loads[2].start()
    loads[3].start()

    barrier = pltpu.get_barrier_semaphore()
    for step in range(1, groups):
        pl.semaphore_signal(
            barrier, inc=1, device_id={"replica": lax.rem(me + step, groups)}, device_id_type=MESH
        )
    for step in range(1, shards):
        pl.semaphore_signal(
            barrier, inc=1, device_id={"tensor": lax.rem(mine + step, shards)}, device_id_type=MESH
        )

    def table_copy(step):
        return pltpu.make_async_remote_copy(
            src_ref=table.at[me],
            dst_ref=table.at[me],
            send_sem=table_send.at[step],
            recv_sem=table_recv.at[step],
            device_id={"replica": lax.rem(me + step, groups)},
            device_id_type=MESH,
        )

    def length_copy(step):
        return pltpu.make_async_remote_copy(
            src_ref=length.at[me],
            dst_ref=length.at[me],
            send_sem=length_send.at[step],
            recv_sem=length_recv.at[step],
            device_id={"replica": lax.rem(me + step, groups)},
            device_id_type=MESH,
        )

    def q_copy(group, k, way):
        dest = z + (1 if way == 0 else -1)
        return pltpu.make_async_remote_copy(
            src_ref=qall.at[group, k],
            dst_ref=qall.at[group, k],
            send_sem=q_send.at[way, group, k],
            recv_sem=q_recv.at[group, k],
            device_id={"replica": dest * inner + x},
            device_id_type=MESH,
        )

    def page_copy(step, group, k):
        return pltpu.make_async_remote_copy(
            src_ref=outgoing.at[step - 1, group, k],
            dst_ref=arrived.at[step - 1, group, k],
            send_sem=page_send.at[step - 1, group, k],
            recv_sem=page_recv.at[step - 1, group, k],
            device_id={"replica": z * inner + lax.rem(x + step, inner)},
            device_id_type=MESH,
        )

    def back_copy(group, k, source):
        return pltpu.make_async_remote_copy(
            src_ref=back.at[group, k],
            dst_ref=came.at[source, k],
            send_sem=back_send.at[group, k],
            recv_sem=back_recv.at[source, k],
            device_id={"replica": group * inner + x},
            device_id_type=MESH,
        )

    def log_copy(group, k, source):
        return pltpu.make_async_remote_copy(
            src_ref=back_log.at[group, k],
            dst_ref=came_log.at[source, k],
            send_sem=log_send.at[group, k],
            recv_sem=log_recv.at[source, k],
            device_id={"replica": group * inner + x},
            device_id_type=MESH,
        )

    def weight_copy(index):
        return pltpu.make_async_copy(
            weight.at[:, pl.ds(pl.multiple_of(index * tile, tile), tile)],
            wbuf.at[index],
            weight_sem.at[index],
        )

    def core_copy(index):
        return pltpu.make_async_remote_copy(
            src_ref=part.at[index, 1 - core],
            dst_ref=sibling.at[index],
            send_sem=core_send.at[index],
            recv_sem=core_recv.at[index],
            device_id={"tensor": chip * CORES + 1 - core},
            device_id_type=MESH,
        )

    def part_copy(index, step):
        dest = lax.rem(chip + step, chips)
        return pltpu.make_async_remote_copy(
            src_ref=joined.at[index, step - 1],
            dst_ref=landed.at[index, step - 1],
            send_sem=part_send.at[index, step - 1],
            recv_sem=part_recv.at[index, step - 1],
            device_id={"tensor": dest * CORES + core},
            device_id_type=MESH,
        )

    perm[...] = selection(block, kv_count)

    side = z // half

    def served(turn):
        across = (1 - side) * (half + turn) + side * (half - 1 - turn)
        beside = side * half + lax.rem(z - side * half + 1 + turn - half + outer, half)
        far = (turn < half).astype(jnp.int32) if not isinstance(turn, int) else int(turn < half)
        return far * across + (1 - far) * beside

    loads[0].wait()
    loads[1].wait()
    pl.semaphore_wait(barrier, groups + shards - 2)
    for step in range(1, groups):
        table_copy(step).start()
        length_copy(step).start()
    for copy in q_loads:
        copy.wait()
    for k in range(kv_count):
        @pl.when(z < outer - 1)
        def _():
            q_copy(z, k, 0).start()

        @pl.when(z > 0)
        def _():
            q_copy(z, k, 1).start()

    loads[2].wait()
    loads[3].wait()

    def request(group, owner):
        count = jnp.int32(0)
        zero = jnp.int32(0)
        shelf, dialog, fill = [zero] * SLOT, [zero] * SLOT, [zero] * SLOT
        low = owner * pool_size
        for d in range(dialogs):
            total = length[group, d]
            for e in range(entries):
                place = table[group, d, e] - low
                live = jnp.minimum(total - e * PAGE, PAGE)
                hit = (place >= 0) & (place < pool_size) & (live > 0)
                for s in range(SLOT):
                    here = hit & (count == s)
                    shelf[s] = jnp.where(here, place, shelf[s])
                    dialog[s] = jnp.where(here, d, dialog[s])
                    fill[s] = jnp.where(here, live, fill[s])
                count = count + hit.astype(jnp.int32)
        return shelf, dialog, fill

    def await_tables(group):
        for other in range(inner):
            source = group * inner + other
            step = lax.rem(me - source + groups, groups)

            @pl.when(source != me)
            def _():
                table_copy(step).wait_recv()
                length_copy(step).wait_recv()

    def separate(shelf, put):
        for s in range(SLOT):
            for b in range(page_rows // block):
                split = jnp.dot(
                    perm[...],
                    pool_ref[shelf[s], b * block : (b + 1) * block, :],
                    preferred_element_type=jnp.float32,
                ).astype(jnp.bfloat16)
                for k in range(kv_count):
                    for kind in range(2):
                        low = (2 * k + kind) * block_tokens
                        put(k, s, kind, b * block_tokens, split[low : low + block_tokens])

    def relay(distance, k):
        @pl.when(z >= distance)
        def _():
            q_copy(z - distance, k, 0).wait_recv()

        @pl.when((z >= distance) & (z < outer - 1))
        def _():
            q_copy(z - distance, k, 0).start()

        @pl.when(z < outer - distance)
        def _():
            q_copy(z + distance, k, 1).wait_recv()

        @pl.when((z < outer - distance) & (z > 0))
        def _():
            q_copy(z + distance, k, 1).start()

    def send_pages(turn, carry):
        group = served(turn)
        await_tables(group)
        for step in range(1, inner):
            shelf, _, _ = request(group * inner + lax.rem(x + step, inner), me)

            def put(k, s, kind, at, rows_of):
                outgoing[step - 1, group, k, s, kind, at : at + block_tokens, :] = rows_of

            separate(shelf, put)
            for k in range(kv_count):
                page_copy(step, group, k).start()
        return carry

    lax.fori_loop(0, 1, send_pages, 0)
    for distance in range(1, half):
        relay(distance, 0)
    lax.fori_loop(1, outer, send_pages, 0)

    for index in range(tiles):
        weight_copy(index).start()

    def list_pages(group, carry):
        for step in range(inner):
            shelf, dialog, fill = request(
                group * inner + x, z * inner + lax.rem(x - step + inner, inner)
            )
            for s in range(SLOT):
                listed[group, step, s, 0] = dialog[s]
                listed[group, step, s, 1] = fill[s]
            if step == 0:

                def put(k, s, kind, at, rows_of):
                    kept[group, k, s, kind, at : at + block_tokens, :] = rows_of

                separate(shelf, put)
        return carry

    lax.fori_loop(0, half, list_pages, 0)
    for k in range(1, kv_count):
        for distance in range(1, half):
            relay(distance, k)
    lax.fori_loop(half, outer, list_pages, 0)

    fresh_rows = fresh_ref.shape[0]
    split = jnp.dot(
        selection(fresh_rows, kv_count), fresh_ref[...], preferred_element_type=jnp.float32
    ).astype(jnp.bfloat16)
    row_token = lax.broadcasted_iota(jnp.int32, (rows, token_rows), 0) % new_len
    col_token = lax.broadcasted_iota(jnp.int32, (rows, token_rows), 1)
    for k in range(kv_count):
        keys = split[(2 * k) * token_rows : (2 * k + 1) * token_rows]
        values = split[(2 * k + 1) * token_rows : (2 * k + 2) * token_rows]
        for d in range(dialogs):
            scores = lax.dot_general(
                qall[z, k, d], keys, CONTRACT, preferred_element_type=jnp.float32
            ) * scale
            causal = (col_token // new_len == d) & (col_token - d * new_len <= row_token)
            scores = jnp.where(causal, scores, floor_value)
            peak = jnp.max(scores, axis=-1, keepdims=True)
            weights = jnp.exp2(scores - peak).astype(jnp.bfloat16)
            peak_ref[z, k, d] = jnp.broadcast_to(peak, (rows, HD))
            amount_ref[z, k, d] = jnp.broadcast_to(
                jnp.sum(weights.astype(jnp.float32), axis=-1, keepdims=True), (rows, HD)
            )
            summed_ref[z, k, d] = jnp.dot(weights, values, preferred_element_type=jnp.float32)

    def absorb(group, k, step, pages, first):
        position = lax.broadcasted_iota(jnp.int32, (rows, PAGE), 1)
        dialog = [listed[group, step, s, 0] for s in range(SLOT)]
        fill = [listed[group, step, s, 1] for s in range(SLOT)]
        owned = [
            [jnp.broadcast_to(dialog[s], (rows, HD)) == d for d in range(dialogs)]
            for s in range(SLOT)
        ]
        for d in range(dialogs):
            qcur[d] = qall[group, k, d]
        scores, highs = [], []
        for s in range(SLOT):
            found = lax.dot_general(
                qcur[dialog[s]], pages[s, 0], CONTRACT, preferred_element_type=jnp.float32
            ) * scale
            found = jnp.where(position < fill[s], found, floor_value)
            scores.append(found)
            highs.append(jnp.broadcast_to(jnp.max(found, axis=-1, keepdims=True), (rows, HD)))
        peaks, keeps = [], []
        for d in range(dialogs):
            peak = functools.reduce(
                jnp.maximum,
                [jnp.where(owned[s][d], highs[s], floor_value) for s in range(SLOT)],
            )
            if not first:
                before = peak_ref[group, k, d]
                peak = jnp.maximum(peak, before)
                keeps.append(jnp.exp2(before - peak))
            peaks.append(peak)
            peak_ref[group, k, d] = peak
        amounts, sums = [], []
        for s in range(SLOT):
            peak = peaks[-1]
            for d in reversed(range(dialogs - 1)):
                peak = jnp.where(owned[s][d], peaks[d], peak)
            weights = jnp.exp2(scores[s] - peak).astype(jnp.bfloat16)
            amounts.append(
                jnp.broadcast_to(
                    jnp.sum(weights.astype(jnp.float32), axis=-1, keepdims=True), (rows, HD)
                )
            )
            sums.append(jnp.dot(weights, pages[s, 1], preferred_element_type=jnp.float32))
        for d in range(dialogs):
            amount = functools.reduce(
                jnp.add, [jnp.where(owned[s][d], amounts[s], 0.0) for s in range(SLOT)]
            )
            total = functools.reduce(
                jnp.add, [jnp.where(owned[s][d], sums[s], 0.0) for s in range(SLOT)]
            )
            if not first:
                amount = amount + keeps[d] * amount_ref[group, k, d]
                total = total + keeps[d] * summed_ref[group, k, d]
            amount_ref[group, k, d] = amount
            summed_ref[group, k, d] = total

    def absorb_kept(group, k, first):
        absorb(group, k, 0, kept.at[group, k], first)

    def absorb_arrived(group, k):
        for step in range(1, inner):
            page_copy(step, group, k).wait_recv()
            absorb(group, k, step, arrived.at[step - 1, group, k], False)

    def begin(k, carry):
        absorb_kept(z, k, False)
        return carry

    lax.fori_loop(0, kv_count, begin, 0)

    def serve(index, carry):
        group = served(index // kv_count)
        k = index % kv_count
        absorb_kept(group, k, True)
        absorb_arrived(group, k)
        for d in range(dialogs):
            amount = jnp.maximum(amount_ref[group, k, d], tiny_value)
            back[group, k, d] = (summed_ref[group, k, d] / amount).astype(jnp.bfloat16)
            log = peak_ref[group, k, d] + jnp.log2(amount)
            back_log[group, k, d : d + 1, :] = jnp.transpose(log)[:1]
        back_copy(group, k, z).start()
        log_copy(group, k, z).start()
        return carry

    def serve_far(index, carry):
        relay(half + index // kv_count, index % kv_count)
        return serve(index, carry)

    lax.fori_loop(0, half * kv_count, serve_far, 0)
    lax.fori_loop(half * kv_count, (outer - 1) * kv_count, serve, 0)

    def merge(turn, k):
        source = served(turn)
        back_copy(source, k, source).wait_recv()
        log_copy(source, k, source).wait_recv()
        for d in range(dialogs):
            line = came_log[source, k, d : d + 1, :]
            log = jnp.transpose(jnp.broadcast_to(line, (HD, rows)))
            before = peak_ref[z, k, d]
            peak = jnp.maximum(before, log)
            keep = jnp.exp2(before - peak)
            take = jnp.exp2(log - peak)
            peak_ref[z, k, d] = peak
            amount_ref[z, k, d] = keep * amount_ref[z, k, d] + take
            summed_ref[z, k, d] = keep * summed_ref[z, k, d] + take * came[
                source, k, d
            ].astype(jnp.float32)
        return k

    head_depth = per_group * HD

    def complete(k, carry):
        lax.fori_loop(0, half, merge, k)
        absorb_arrived(z, k)
        lax.fori_loop(half, outer - 1, merge, k)
        for d in range(dialogs):
            ratio = (summed_ref[z, k, d] / amount_ref[z, k, d]).astype(jnp.bfloat16)
            for g in range(per_group):
                attended[k, d * new_len : (d + 1) * new_len, g * HD : (g + 1) * HD] = ratio[
                    g * new_len : (g + 1) * new_len
                ]
        return carry

    def product_of(k, index):
        return jnp.dot(
            attended[k],
            wbuf[index, pl.ds(k * head_depth, head_depth), :],
            preferred_element_type=jnp.float32,
        )

    for k in range(kv_count):
        complete(k, 0)
        if k == kv_count - 1:
            break

        def collect(index, carry):
            if k == 0:
                weight_copy(index).wait()
                gathered[index] = product_of(k, index)
            else:
                gathered[index] += product_of(k, index)
            return carry

        lax.fori_loop(0, tiles, collect, 0)

    def join(index):
        core_copy(index).wait_recv()
        for step in range(1, chips):
            dest = lax.rem(chip + step, chips)
            total = part[index, core, dest].astype(jnp.float32) + sibling[index, dest].astype(
                jnp.float32
            )
            joined[index, step - 1] = total.astype(jnp.bfloat16)
            part_copy(index, step).start()

    def project(index, carry):
        if kv_count == 1:
            weight_copy(index).wait()
        product = product_of(kv_count - 1, index)
        if kv_count > 1:
            product = product + gathered[index]
        product = product.astype(jnp.bfloat16)
        for dest in range(shards):
            part[index, dest % CORES, dest // CORES] = product[
                dest * block_rows : (dest + 1) * block_rows
            ]
        core_copy(index).start()

        @pl.when(index >= LAG)
        def _():
            join(index - LAG)

        return carry

    lax.fori_loop(0, tiles, project, 0)

    def join_rest(index, carry):
        join(index)
        return carry

    lax.fori_loop(max(tiles - LAG, 0), tiles, join_rest, 0)

    def finish(index, carry):
        total = part[index, core, chip].astype(jnp.float32) + sibling[index, chip].astype(
            jnp.float32
        )
        for step in range(1, chips):
            part_copy(index, step).wait_recv()
            total = total + landed[index, step - 1].astype(jnp.float32)
        out_ref[:, pl.ds(pl.multiple_of(index * tile, tile), tile)] = total.astype(out_ref.dtype)
        return carry

    lax.fori_loop(0, tiles, finish, 0)

    def drain(index, carry):
        core_copy(index).wait_send()
        for step in range(1, chips):
            part_copy(index, step).wait_send()
        return carry

    lax.fori_loop(0, tiles, drain, 0)

    def drain_back(turn, carry):
        for k in range(kv_count):
            back_copy(served(turn), k, z).wait_send()
            log_copy(served(turn), k, z).wait_send()
        return carry

    lax.fori_loop(0, outer - 1, drain_back, 0)

    def drain_line(group, carry):
        for k in range(kv_count):
            for step in range(1, inner):
                page_copy(step, group, k).wait_send()

            @pl.when((group <= z) & (z < outer - 1))
            def _():
                q_copy(group, k, 0).wait_send()

            @pl.when((group >= z) & (z > 0))
            def _():
                q_copy(group, k, 1).wait_send()

        return carry

    lax.fori_loop(0, outer, drain_line, 0)
    for step in range(1, groups):
        table_copy(step).wait_send()
        length_copy(step).wait_send()


def local(queries, kv_new, pool, page_table, hist_len, o_weight):
    groups = lax.axis_size("replica")
    shards = lax.axis_size("tensor")
    outer, inner = spread(groups)
    pool_size, page_len, _, kv_width = pool.shape
    dialogs, entries = page_table.shape
    token_rows = queries.shape[0]
    new_len = token_rows // dialogs
    kv_count = kv_width // HD
    per_group = queries.shape[1] // kv_width
    rows = per_group * new_len
    depth, model = o_weight.shape
    tile = min(TILE, model)
    tiles = model // tile
    block_rows = token_rows // shards
    chips = shards // CORES
    page_rows = 2 * kv_count * page_len
    block = 256
    pages = pool.reshape(pool_size, page_len, 2, kv_count, HD).transpose(0, 1, 3, 2, 4)
    pages = pages.reshape(pool_size, page_rows, HD)
    fresh = kv_new.reshape(token_rows, 2, kv_count, HD).transpose(0, 2, 1, 3)
    fresh = fresh.reshape(2 * kv_count * token_rows, HD)
    vmem = pl.BlockSpec(memory_space=pltpu.VMEM)
    anywhere = pl.BlockSpec(memory_space=pl.ANY)
    dma = pltpu.SemaphoreType.DMA
    bf16, f32 = jnp.bfloat16, jnp.float32
    return pl.pallas_call(
        functools.partial(kernel, groups, shards),
        out_shape=jax.ShapeDtypeStruct((block_rows, model), jnp.bfloat16),
        in_specs=[anywhere] * 6,
        out_specs=vmem,
        scratch_shapes=[
            pltpu.SMEM((groups, dialogs, entries), jnp.int32),
            pltpu.SMEM((groups, dialogs), jnp.int32),
            pltpu.SMEM((outer, inner, SLOT, 2), jnp.int32),
            pltpu.VMEM((pool_size, page_rows, HD), bf16),
            pltpu.VMEM((2 * kv_count * token_rows, HD), bf16),
            pltpu.VMEM((outer, kv_count, SLOT, 2, page_len, HD), bf16),
            pltpu.VMEM((inner - 1, outer, kv_count, SLOT, 2, page_len, HD), bf16),
            pltpu.VMEM((inner - 1, outer, kv_count, SLOT, 2, page_len, HD), bf16),
            pltpu.VMEM((tiles, depth, tile), bf16),
            pltpu.VMEM((block, block), bf16),
            pltpu.VMEM((outer, kv_count, dialogs, rows, HD), bf16),
            pltpu.VMEM((dialogs, rows, HD), bf16),
            pltpu.VMEM((outer, kv_count, dialogs, rows, HD), f32),
            pltpu.VMEM((outer, kv_count, dialogs, rows, HD), f32),
            pltpu.VMEM((outer, kv_count, dialogs, rows, HD), f32),
            pltpu.VMEM((outer, kv_count, dialogs, rows, HD), bf16),
            pltpu.VMEM((outer, kv_count, dialogs, rows), f32),
            pltpu.VMEM((outer, kv_count, dialogs, rows, HD), bf16),
            pltpu.VMEM((outer, kv_count, dialogs, rows), f32),
            pltpu.VMEM((kv_count, token_rows, depth // kv_count), bf16),
            pltpu.VMEM((tiles, token_rows, tile), f32),
            pltpu.VMEM((tiles, CORES, chips, block_rows, tile), bf16),
            pltpu.VMEM((tiles, chips, block_rows, tile), bf16),
            pltpu.VMEM((tiles, chips - 1, block_rows, tile), bf16),
            pltpu.VMEM((tiles, chips - 1, block_rows, tile), bf16),
            dma((4,)),
            dma((kv_count, dialogs, per_group)),
            dma((tiles,)),
            dma((groups,)),
            dma((groups,)),
            dma((groups,)),
            dma((groups,)),
            dma((2, outer, kv_count)),
            dma((outer, kv_count)),
            dma((inner - 1, outer, kv_count)),
            dma((inner - 1, outer, kv_count)),
            dma((outer, kv_count)),
            dma((outer, kv_count)),
            dma((outer, kv_count)),
            dma((outer, kv_count)),
            dma((tiles,)),
            dma((tiles,)),
            dma((tiles, chips - 1)),
            dma((tiles, chips - 1)),
        ],
        compiler_params=pltpu.CompilerParams(
            collective_id=0, has_side_effects=True, vmem_limit_bytes=63 * 1024 * 1024
        ),
        name="attend",
    )(queries, fresh, pages, page_table, hist_len, o_weight)


def solution(mesh):
    in_specs = (
        P("replica", "tensor"),
        P("replica", None, "tensor"),
        P("replica", None, None, "tensor"),
        P("replica", None),
        P("replica"),
        P("tensor", None),
    )
    out_specs = P(("replica", "tensor"), None)
    return jax.shard_map(local, mesh=mesh, in_specs=in_specs, out_specs=out_specs, check_vma=False)
```

```python
import functools
import math

import jax
import jax.numpy as jnp
from jax import lax
from jax.experimental import pallas as pl
from jax.experimental.pallas import tpu as pltpu
from jax.sharding import PartitionSpec as P

HD = 128
PAGE = 128
SLOT = 3
TILE = 2048
LAG = 1
CORES = 2

BATCH = 2

floor_value = -1e30
tiny_value = 1e-30

MESH = pl.DeviceIdType.MESH
CONTRACT = (((1,), (1,)), ((), ()))


def spread(groups):
    outer = 1
    while outer * outer < groups:
        outer *= 2
    return outer, groups // outer


def selection(rows, kv_count):
    kinds = 2 * kv_count
    tokens = rows // kinds
    i = lax.broadcasted_iota(jnp.int32, (rows, rows), 0)
    j = lax.broadcasted_iota(jnp.int32, (rows, rows), 1)
    source = (i % tokens) * kinds + i // tokens
    return jnp.where(source == j, 1.0, 0.0).astype(jnp.bfloat16)


def kernel(
    groups, shards,
    q_hbm, fresh_hbm, pool_hbm, table_hbm, length_hbm, weight,
    out_ref,
    table, length, listed, pool_ref, fresh_ref, kept, outgoing, arrived, wbuf, perm, qall, qcur,
    peak_ref, amount_ref, summed_ref, back, back_log, came, came_log, attended, gathered,
    part, sibling, joined, landed,
    load_sem, q_load_sem, weight_sem,
    table_send, table_recv, length_send, length_recv,
    q_send, q_recv, page_send, page_recv,
    back_send, back_recv, log_send, log_recv,
    core_send, core_recv, part_send, part_recv,
):
    outer, inner = spread(groups)
    half = outer // 2
    me = lax.axis_index("replica")
    mine = lax.axis_index("tensor")
    z = me // inner
    x = me % inner
    pool_size = pool_ref.shape[0]
    _, kv_count, dialogs, rows, _ = qall.shape
    entries = table.shape[2]
    token_rows = q_hbm.shape[0]
    new_len = token_rows // dialogs
    per_group = rows // new_len
    tiles, _, chips, block_rows, tile = part.shape
    block = perm.shape[0]
    page_rows = pool_ref.shape[1]
    block_tokens = block // (2 * kv_count)
    scale = math.log2(math.e) / math.sqrt(HD)
    chip = mine // CORES
    core = mine % CORES

    loads = [
        pltpu.make_async_copy(table_hbm, table.at[me], load_sem.at[0]),
        pltpu.make_async_copy(length_hbm, length.at[me], load_sem.at[1]),
        pltpu.make_async_copy(pool_hbm, pool_ref, load_sem.at[2]),
        pltpu.make_async_copy(fresh_hbm, fresh_ref, load_sem.at[3]),
    ]

    def q_load(k, d, g):
        col = (k * per_group + g) * HD
        return pltpu.make_async_copy(
            q_hbm.at[d * new_len : (d + 1) * new_len, col : col + HD],
            qall.at[z, k, d, g * new_len : (g + 1) * new_len, :],
            q_load_sem.at[k, d, g],
        )

    q_loads = [
        q_load(k, d, g) for k in range(kv_count) for d in range(dialogs) for g in range(per_group)
    ]

    loads[0].start()
    loads[1].start()
    for copy in q_loads:
        copy.start()
    loads[2].start()
    loads[3].start()

    barrier = pltpu.get_barrier_semaphore()
    for step in range(1, groups):
        pl.semaphore_signal(
            barrier, inc=1, device_id={"replica": lax.rem(me + step, groups)}, device_id_type=MESH
        )
    for step in range(1, shards):
        pl.semaphore_signal(
            barrier, inc=1, device_id={"tensor": lax.rem(mine + step, shards)}, device_id_type=MESH
        )

    def table_copy(step):
        return pltpu.make_async_remote_copy(
            src_ref=table.at[me],
            dst_ref=table.at[me],
            send_sem=table_send.at[step],
            recv_sem=table_recv.at[step],
            device_id={"replica": lax.rem(me + step, groups)},
            device_id_type=MESH,
        )

    def length_copy(step):
        return pltpu.make_async_remote_copy(
            src_ref=length.at[me],
            dst_ref=length.at[me],
            send_sem=length_send.at[step],
            recv_sem=length_recv.at[step],
            device_id={"replica": lax.rem(me + step, groups)},
            device_id_type=MESH,
        )

    def q_copy(group, k, way):
        dest = z + (1 if way == 0 else -1)
        return pltpu.make_async_remote_copy(
            src_ref=qall.at[group, k],
            dst_ref=qall.at[group, k],
            send_sem=q_send.at[way, group, k],
            recv_sem=q_recv.at[group, k],
            device_id={"replica": dest * inner + x},
            device_id_type=MESH,
        )

    def page_copy(step, group, k):
        return pltpu.make_async_remote_copy(
            src_ref=outgoing.at[step - 1, group, k],
            dst_ref=arrived.at[step - 1, group, k],
            send_sem=page_send.at[step - 1, group, k],
            recv_sem=page_recv.at[step - 1, group, k],
            device_id={"replica": z * inner + lax.rem(x + step, inner)},
            device_id_type=MESH,
        )

    def back_copy(group, k, source):
        return pltpu.make_async_remote_copy(
            src_ref=back.at[group, k],
            dst_ref=came.at[source, k],
            send_sem=back_send.at[group, k],
            recv_sem=back_recv.at[source, k],
            device_id={"replica": group * inner + x},
            device_id_type=MESH,
        )

    def log_copy(group, k, source):
        return pltpu.make_async_remote_copy(
            src_ref=back_log.at[group, k],
            dst_ref=came_log.at[source, k],
            send_sem=log_send.at[group, k],
            recv_sem=log_recv.at[source, k],
            device_id={"replica": group * inner + x},
            device_id_type=MESH,
        )

    def weight_copy(index):
        return pltpu.make_async_copy(
            weight.at[:, pl.ds(pl.multiple_of(index * tile, tile), tile)],
            wbuf.at[index],
            weight_sem.at[index],
        )

    def core_copy(index):
        return pltpu.make_async_remote_copy(
            src_ref=part.at[index, 1 - core],
            dst_ref=sibling.at[index],
            send_sem=core_send.at[index],
            recv_sem=core_recv.at[index],
            device_id={"tensor": chip * CORES + 1 - core},
            device_id_type=MESH,
        )

    def part_copy(index, step):
        dest = lax.rem(chip + step, chips)
        return pltpu.make_async_remote_copy(
            src_ref=joined.at[index, step - 1],
            dst_ref=landed.at[index, step - 1],
            send_sem=part_send.at[index, step - 1],
            recv_sem=part_recv.at[index, step - 1],
            device_id={"tensor": dest * CORES + core},
            device_id_type=MESH,
        )

    perm[...] = selection(block, kv_count)

    side = z // half

    def served(turn):
        across = (1 - side) * (half + turn) + side * (half - 1 - turn)
        beside = side * half + lax.rem(z - side * half + 1 + turn - half + outer, half)
        far = (turn < half).astype(jnp.int32) if not isinstance(turn, int) else int(turn < half)
        return far * across + (1 - far) * beside

    loads[0].wait()
    loads[1].wait()
    pl.semaphore_wait(barrier, groups + shards - 2)
    for step in range(1, groups):
        table_copy(step).start()
        length_copy(step).start()
    for copy in q_loads:
        copy.wait()
    for k in range(kv_count):
        @pl.when(z < outer - 1)
        def _():
            q_copy(z, k, 0).start()

        @pl.when(z > 0)
        def _():
            q_copy(z, k, 1).start()

    loads[2].wait()
    loads[3].wait()

    def request(group, owner):
        count = jnp.int32(0)
        zero = jnp.int32(0)
        shelf, dialog, fill = [zero] * SLOT, [zero] * SLOT, [zero] * SLOT
        low = owner * pool_size
        for d in range(dialogs):
            total = length[group, d]
            for e in range(entries):
                place = table[group, d, e] - low
                live = jnp.minimum(total - e * PAGE, PAGE)
                hit = (place >= 0) & (place < pool_size) & (live > 0)
                for s in range(SLOT):
                    here = hit & (count == s)
                    shelf[s] = jnp.where(here, place, shelf[s])
                    dialog[s] = jnp.where(here, d, dialog[s])
                    fill[s] = jnp.where(here, live, fill[s])
                count = count + hit.astype(jnp.int32)
        return shelf, dialog, fill

    def await_tables(group):
        for other in range(inner):
            source = group * inner + other
            step = lax.rem(me - source + groups, groups)

            @pl.when(source != me)
            def _():
                table_copy(step).wait_recv()
                length_copy(step).wait_recv()

    def separate(shelf, put):
        for s in range(SLOT):
            for b in range(page_rows // block):
                split = jnp.dot(
                    perm[...],
                    pool_ref[shelf[s], b * block : (b + 1) * block, :],
                    preferred_element_type=jnp.float32,
                ).astype(jnp.bfloat16)
                for k in range(kv_count):
                    for kind in range(2):
                        low = (2 * k + kind) * block_tokens
                        put(k, s, kind, b * block_tokens, split[low : low + block_tokens])

    def relay(distance, k):
        @pl.when(z >= distance)
        def _():
            q_copy(z - distance, k, 0).wait_recv()

        @pl.when((z >= distance) & (z < outer - 1))
        def _():
            q_copy(z - distance, k, 0).start()

        @pl.when(z < outer - distance)
        def _():
            q_copy(z + distance, k, 1).wait_recv()

        @pl.when((z < outer - distance) & (z > 0))
        def _():
            q_copy(z + distance, k, 1).start()

    def send_pages(turn, carry):
        group = served(turn)
        await_tables(group)
        for step in range(1, inner):
            shelf, _, _ = request(group * inner + lax.rem(x + step, inner), me)

            def put(k, s, kind, at, rows_of):
                outgoing[step - 1, group, k, s, kind, at : at + block_tokens, :] = rows_of

            separate(shelf, put)
            for k in range(kv_count):
                page_copy(step, group, k).start()
        return carry

    lax.fori_loop(0, 1, send_pages, 0)
    for distance in range(1, half):
        relay(distance, 0)
    lax.fori_loop(1, outer, send_pages, 0)

    for index in range(tiles):
        weight_copy(index).start()

    def list_pages(group, carry):
        for step in range(inner):
            shelf, dialog, fill = request(
                group * inner + x, z * inner + lax.rem(x - step + inner, inner)
            )
            for s in range(SLOT):
                listed[group, step, s, 0] = dialog[s]
                listed[group, step, s, 1] = fill[s]
            if step == 0:

                def put(k, s, kind, at, rows_of):
                    kept[group, k, s, kind, at : at + block_tokens, :] = rows_of

                separate(shelf, put)
        return carry

    lax.fori_loop(0, half, list_pages, 0)
    for k in range(1, kv_count):
        for distance in range(1, half):
            relay(distance, k)
    lax.fori_loop(half, outer, list_pages, 0)

    fresh_rows = fresh_ref.shape[0]
    split = jnp.dot(
        selection(fresh_rows, kv_count), fresh_ref[...], preferred_element_type=jnp.float32
    ).astype(jnp.bfloat16)
    row_token = lax.broadcasted_iota(jnp.int32, (rows, token_rows), 0) % new_len
    col_token = lax.broadcasted_iota(jnp.int32, (rows, token_rows), 1)
    for k in range(kv_count):
        keys = split[(2 * k) * token_rows : (2 * k + 1) * token_rows]
        values = split[(2 * k + 1) * token_rows : (2 * k + 2) * token_rows]
        for d in range(dialogs):
            scores = lax.dot_general(
                qall[z, k, d], keys, CONTRACT, preferred_element_type=jnp.float32
            ) * scale
            causal = (col_token // new_len == d) & (col_token - d * new_len <= row_token)
            scores = jnp.where(causal, scores, floor_value)
            peak = jnp.max(scores, axis=-1, keepdims=True)
            weights = jnp.exp2(scores - peak).astype(jnp.bfloat16)
            peak_ref[z, k, d] = jnp.broadcast_to(peak, (rows, HD))
            amount_ref[z, k, d] = jnp.broadcast_to(
                jnp.sum(weights.astype(jnp.float32), axis=-1, keepdims=True), (rows, HD)
            )
            summed_ref[z, k, d] = jnp.dot(weights, values, preferred_element_type=jnp.float32)

    def absorb(group, k, step, pages, first):
        position = lax.broadcasted_iota(jnp.int32, (rows, PAGE), 1)
        dialog = [listed[group, step, s, 0] for s in range(SLOT)]
        fill = [listed[group, step, s, 1] for s in range(SLOT)]
        owned = [
            [jnp.broadcast_to(dialog[s], (rows, HD)) == d for d in range(dialogs)]
            for s in range(SLOT)
        ]
        for d in range(dialogs):
            qcur[d] = qall[group, k, d]
        scores, highs = [], []
        for s in range(SLOT):
            found = lax.dot_general(
                qcur[dialog[s]], pages[s, 0], CONTRACT, preferred_element_type=jnp.float32
            ) * scale
            found = jnp.where(position < fill[s], found, floor_value)
            scores.append(found)
            highs.append(jnp.broadcast_to(jnp.max(found, axis=-1, keepdims=True), (rows, HD)))
        peaks, keeps = [], []
        for d in range(dialogs):
            peak = functools.reduce(
                jnp.maximum,
                [jnp.where(owned[s][d], highs[s], floor_value) for s in range(SLOT)],
            )
            if not first:
                before = peak_ref[group, k, d]
                peak = jnp.maximum(peak, before)
                keeps.append(jnp.exp2(before - peak))
            peaks.append(peak)
            peak_ref[group, k, d] = peak
        amounts, sums = [], []
        for s in range(SLOT):
            peak = peaks[-1]
            for d in reversed(range(dialogs - 1)):
                peak = jnp.where(owned[s][d], peaks[d], peak)
            weights = jnp.exp2(scores[s] - peak).astype(jnp.bfloat16)
            amounts.append(
                jnp.broadcast_to(
                    jnp.sum(weights.astype(jnp.float32), axis=-1, keepdims=True), (rows, HD)
                )
            )
            sums.append(jnp.dot(weights, pages[s, 1], preferred_element_type=jnp.float32))
        for d in range(dialogs):
            amount = functools.reduce(
                jnp.add, [jnp.where(owned[s][d], amounts[s], 0.0) for s in range(SLOT)]
            )
            total = functools.reduce(
                jnp.add, [jnp.where(owned[s][d], sums[s], 0.0) for s in range(SLOT)]
            )
            if not first:
                amount = amount + keeps[d] * amount_ref[group, k, d]
                total = total + keeps[d] * summed_ref[group, k, d]
            amount_ref[group, k, d] = amount
            summed_ref[group, k, d] = total

    def absorb_kept(group, k, first):
        absorb(group, k, 0, kept.at[group, k], first)

    def absorb_arrived(group, k):
        for step in range(1, inner):
            page_copy(step, group, k).wait_recv()
            absorb(group, k, step, arrived.at[step - 1, group, k], False)

    def begin(k, carry):
        absorb_kept(z, k, False)
        return carry

    lax.fori_loop(0, kv_count, begin, 0)

    def serve(index, carry):
        group = served(index // kv_count)
        k = index % kv_count
        absorb_kept(group, k, True)
        absorb_arrived(group, k)
        for d in range(dialogs):
            amount = jnp.maximum(amount_ref[group, k, d], tiny_value)
            back[group, k, d] = (summed_ref[group, k, d] / amount).astype(jnp.bfloat16)
            log = peak_ref[group, k, d] + jnp.log2(amount)
            back_log[group, k, d : d + 1, :] = jnp.transpose(log)[:1]
        back_copy(group, k, z).start()
        log_copy(group, k, z).start()
        return carry

    def serve_far(index, carry):
        relay(half + index // kv_count, index % kv_count)
        return serve(index, carry)

    lax.fori_loop(0, half * kv_count, serve_far, 0)
    lax.fori_loop(half * kv_count, (outer - 1) * kv_count, serve, 0)

    def merge(turn, k):
        source = served(turn)
        back_copy(source, k, source).wait_recv()
        log_copy(source, k, source).wait_recv()
        for d in range(dialogs):
            line = came_log[source, k, d : d + 1, :]
            log = jnp.transpose(jnp.broadcast_to(line, (HD, rows)))
            before = peak_ref[z, k, d]
            peak = jnp.maximum(before, log)
            keep = jnp.exp2(before - peak)
            take = jnp.exp2(log - peak)
            peak_ref[z, k, d] = peak
            amount_ref[z, k, d] = keep * amount_ref[z, k, d] + take
            summed_ref[z, k, d] = keep * summed_ref[z, k, d] + take * came[
                source, k, d
            ].astype(jnp.float32)
        return k

    head_depth = per_group * HD
    batch = math.gcd(tiles, BATCH)

    def complete(k, carry):
        lax.fori_loop(0, half, merge, k)
        absorb_arrived(z, k)
        lax.fori_loop(half, outer - 1, merge, k)
        for d in range(dialogs):
            ratio = (summed_ref[z, k, d] / amount_ref[z, k, d]).astype(jnp.bfloat16)
            for g in range(per_group):
                attended[k, d * new_len : (d + 1) * new_len, g * HD : (g + 1) * HD] = ratio[
                    g * new_len : (g + 1) * new_len
                ]
        return carry

    def product_of(k, index):
        return jnp.dot(
            attended[k],
            wbuf[index, pl.ds(k * head_depth, head_depth), :],
            preferred_element_type=jnp.float32,
        )

    for k in range(kv_count):
        complete(k, 0)
        if k == kv_count - 1:
            break

        def collect(turn, carry):
            for offset in range(batch):
                index = turn * batch + offset
                if k == 0:
                    weight_copy(index).wait()
                    gathered[index] = product_of(k, index)
                else:
                    gathered[index] += product_of(k, index)
            return carry

        lax.fori_loop(0, tiles // batch, collect, 0)

    def join(index):
        core_copy(index).wait_recv()
        for step in range(1, chips):
            dest = lax.rem(chip + step, chips)
            total = part[index, core, dest].astype(jnp.float32) + sibling[index, dest].astype(
                jnp.float32
            )
            joined[index, step - 1] = total.astype(jnp.bfloat16)
            part_copy(index, step).start()

    def project(index, carry):
        if kv_count == 1:
            weight_copy(index).wait()
        product = product_of(kv_count - 1, index)
        if kv_count > 1:
            product = product + gathered[index]
        product = product.astype(jnp.bfloat16)
        for dest in range(shards):
            part[index, dest % CORES, dest // CORES] = product[
                dest * block_rows : (dest + 1) * block_rows
            ]
        core_copy(index).start()

        @pl.when(index >= LAG)
        def _():
            join(index - LAG)

        return carry

    lax.fori_loop(0, tiles, project, 0)

    def join_rest(index, carry):
        join(index)
        return carry

    lax.fori_loop(max(tiles - LAG, 0), tiles, join_rest, 0)

    def finish(index, carry):
        total = part[index, core, chip].astype(jnp.float32) + sibling[index, chip].astype(
            jnp.float32
        )
        for step in range(1, chips):
            part_copy(index, step).wait_recv()
            total = total + landed[index, step - 1].astype(jnp.float32)
        out_ref[:, pl.ds(pl.multiple_of(index * tile, tile), tile)] = total.astype(out_ref.dtype)
        return carry

    lax.fori_loop(0, tiles, finish, 0)

    def drain(index, carry):
        core_copy(index).wait_send()
        for step in range(1, chips):
            part_copy(index, step).wait_send()
        return carry

    lax.fori_loop(0, tiles, drain, 0)

    def drain_back(turn, carry):
        for k in range(kv_count):
            back_copy(served(turn), k, z).wait_send()
            log_copy(served(turn), k, z).wait_send()
        return carry

    lax.fori_loop(0, outer - 1, drain_back, 0)

    def drain_line(group, carry):
        for k in range(kv_count):
            for step in range(1, inner):
                page_copy(step, group, k).wait_send()

            @pl.when((group <= z) & (z < outer - 1))
            def _():
                q_copy(group, k, 0).wait_send()

            @pl.when((group >= z) & (z > 0))
            def _():
                q_copy(group, k, 1).wait_send()

        return carry

    lax.fori_loop(0, outer, drain_line, 0)
    for step in range(1, groups):
        table_copy(step).wait_send()
        length_copy(step).wait_send()


def local(queries, kv_new, pool, page_table, hist_len, o_weight):
    groups = lax.axis_size("replica")
    shards = lax.axis_size("tensor")
    outer, inner = spread(groups)
    pool_size, page_len, _, kv_width = pool.shape
    dialogs, entries = page_table.shape
    token_rows = queries.shape[0]
    new_len = token_rows // dialogs
    kv_count = kv_width // HD
    per_group = queries.shape[1] // kv_width
    rows = per_group * new_len
    depth, model = o_weight.shape
    tile = min(TILE, model)
    tiles = model // tile
    block_rows = token_rows // shards
    chips = shards // CORES
    page_rows = 2 * kv_count * page_len
    block = 256
    pages = pool.reshape(pool_size, page_len, 2, kv_count, HD).transpose(0, 1, 3, 2, 4)
    pages = pages.reshape(pool_size, page_rows, HD)
    fresh = kv_new.reshape(token_rows, 2, kv_count, HD).transpose(0, 2, 1, 3)
    fresh = fresh.reshape(2 * kv_count * token_rows, HD)
    vmem = pl.BlockSpec(memory_space=pltpu.VMEM)
    anywhere = pl.BlockSpec(memory_space=pl.ANY)
    dma = pltpu.SemaphoreType.DMA
    bf16, f32 = jnp.bfloat16, jnp.float32
    return pl.pallas_call(
        functools.partial(kernel, groups, shards),
        out_shape=jax.ShapeDtypeStruct((block_rows, model), jnp.bfloat16),
        in_specs=[anywhere] * 6,
        out_specs=vmem,
        scratch_shapes=[
            pltpu.SMEM((groups, dialogs, entries), jnp.int32),
            pltpu.SMEM((groups, dialogs), jnp.int32),
            pltpu.SMEM((outer, inner, SLOT, 2), jnp.int32),
            pltpu.VMEM((pool_size, page_rows, HD), bf16),
            pltpu.VMEM((2 * kv_count * token_rows, HD), bf16),
            pltpu.VMEM((outer, kv_count, SLOT, 2, page_len, HD), bf16),
            pltpu.VMEM((inner - 1, outer, kv_count, SLOT, 2, page_len, HD), bf16),
            pltpu.VMEM((inner - 1, outer, kv_count, SLOT, 2, page_len, HD), bf16),
            pltpu.VMEM((tiles, depth, tile), bf16),
            pltpu.VMEM((block, block), bf16),
            pltpu.VMEM((outer, kv_count, dialogs, rows, HD), bf16),
            pltpu.VMEM((dialogs, rows, HD), bf16),
            pltpu.VMEM((outer, kv_count, dialogs, rows, HD), f32),
            pltpu.VMEM((outer, kv_count, dialogs, rows, HD), f32),
            pltpu.VMEM((outer, kv_count, dialogs, rows, HD), f32),
            pltpu.VMEM((outer, kv_count, dialogs, rows, HD), bf16),
            pltpu.VMEM((outer, kv_count, dialogs, rows), f32),
            pltpu.VMEM((outer, kv_count, dialogs, rows, HD), bf16),
            pltpu.VMEM((outer, kv_count, dialogs, rows), f32),
            pltpu.VMEM((kv_count, token_rows, depth // kv_count), bf16),
            pltpu.VMEM((tiles, token_rows, tile), f32),
            pltpu.VMEM((tiles, CORES, chips, block_rows, tile), bf16),
            pltpu.VMEM((tiles, chips, block_rows, tile), bf16),
            pltpu.VMEM((tiles, chips - 1, block_rows, tile), bf16),
            pltpu.VMEM((tiles, chips - 1, block_rows, tile), bf16),
            dma((4,)),
            dma((kv_count, dialogs, per_group)),
            dma((tiles,)),
            dma((groups,)),
            dma((groups,)),
            dma((groups,)),
            dma((groups,)),
            dma((2, outer, kv_count)),
            dma((outer, kv_count)),
            dma((inner - 1, outer, kv_count)),
            dma((inner - 1, outer, kv_count)),
            dma((outer, kv_count)),
            dma((outer, kv_count)),
            dma((outer, kv_count)),
            dma((outer, kv_count)),
            dma((tiles,)),
            dma((tiles,)),
            dma((tiles, chips - 1)),
            dma((tiles, chips - 1)),
        ],
        compiler_params=pltpu.CompilerParams(
            collective_id=0, has_side_effects=True, vmem_limit_bytes=63 * 1024 * 1024
        ),
        name="attend",
    )(queries, fresh, pages, page_table, hist_len, o_weight)


def solution(mesh):
    in_specs = (
        P("replica", "tensor"),
        P("replica", None, "tensor"),
        P("replica", None, None, "tensor"),
        P("replica", None),
        P("replica"),
        P("tensor", None),
    )
    out_specs = P(("replica", "tensor"), None)
    return jax.shard_map(local, mesh=mesh, in_specs=in_specs, out_specs=out_specs, check_vma=False)
```

```python
import functools
import math

import jax
import jax.numpy as jnp
from jax import lax
from jax.experimental import pallas as pl
from jax.experimental.pallas import tpu as pltpu
from jax.sharding import PartitionSpec as P

HD = 128
PAGE = 128
SLOT = 3
TILE = 2048
LAG = 1
CORES = 2

BATCH = 2

floor_value = -1e30
tiny_value = 1e-30

MESH = pl.DeviceIdType.MESH
CONTRACT = (((1,), (1,)), ((), ()))


def spread(groups):
    outer = 1
    while outer * outer < groups:
        outer *= 2
    return outer, groups // outer


def selection(rows, kv_count):
    kinds = 2 * kv_count
    tokens = rows // kinds
    i = lax.broadcasted_iota(jnp.int32, (rows, rows), 0)
    j = lax.broadcasted_iota(jnp.int32, (rows, rows), 1)
    source = (i % tokens) * kinds + i // tokens
    return jnp.where(source == j, 1.0, 0.0).astype(jnp.bfloat16)


def kernel(
    groups, shards,
    q_hbm, fresh_hbm, pool_hbm, table_hbm, length_hbm, weight,
    out_ref,
    table, length, listed, pool_ref, fresh_ref, kept, outgoing, arrived, wbuf, perm, qall, qcur,
    peak_ref, amount_ref, summed_ref, back, back_log, came, came_log, attended, gathered,
    part, sibling, joined, landed, result,
    load_sem, q_load_sem, weight_sem, out_sem,
    table_send, table_recv, length_send, length_recv,
    q_send, q_recv, page_send, page_recv,
    back_send, back_recv, log_send, log_recv,
    core_send, core_recv, part_send, part_recv,
):
    outer, inner = spread(groups)
    half = outer // 2
    me = lax.axis_index("replica")
    mine = lax.axis_index("tensor")
    z = me // inner
    x = me % inner
    pool_size = pool_ref.shape[0]
    _, kv_count, dialogs, rows, _ = qall.shape
    entries = table.shape[2]
    token_rows = q_hbm.shape[0]
    new_len = token_rows // dialogs
    per_group = rows // new_len
    tiles, _, chips, block_rows, tile = part.shape
    block = perm.shape[0]
    page_rows = pool_ref.shape[1]
    block_tokens = block // (2 * kv_count)
    scale = math.log2(math.e) / math.sqrt(HD)
    chip = mine // CORES
    core = mine % CORES

    loads = [
        pltpu.make_async_copy(table_hbm, table.at[me], load_sem.at[0]),
        pltpu.make_async_copy(length_hbm, length.at[me], load_sem.at[1]),
        pltpu.make_async_copy(pool_hbm, pool_ref, load_sem.at[2]),
        pltpu.make_async_copy(fresh_hbm, fresh_ref, load_sem.at[3]),
    ]

    def q_load(k, d, g):
        col = (k * per_group + g) * HD
        return pltpu.make_async_copy(
            q_hbm.at[d * new_len : (d + 1) * new_len, col : col + HD],
            qall.at[z, k, d, g * new_len : (g + 1) * new_len, :],
            q_load_sem.at[k, d, g],
        )

    q_loads = [
        q_load(k, d, g) for k in range(kv_count) for d in range(dialogs) for g in range(per_group)
    ]

    loads[0].start()
    loads[1].start()
    for copy in q_loads:
        copy.start()
    loads[2].start()
    loads[3].start()

    barrier = pltpu.get_barrier_semaphore()
    for step in range(1, groups):
        pl.semaphore_signal(
            barrier, inc=1, device_id={"replica": lax.rem(me + step, groups)}, device_id_type=MESH
        )
    for step in range(1, shards):
        pl.semaphore_signal(
            barrier, inc=1, device_id={"tensor": lax.rem(mine + step, shards)}, device_id_type=MESH
        )

    def table_copy(step):
        return pltpu.make_async_remote_copy(
            src_ref=table.at[me],
            dst_ref=table.at[me],
            send_sem=table_send.at[step],
            recv_sem=table_recv.at[step],
            device_id={"replica": lax.rem(me + step, groups)},
            device_id_type=MESH,
        )

    def length_copy(step):
        return pltpu.make_async_remote_copy(
            src_ref=length.at[me],
            dst_ref=length.at[me],
            send_sem=length_send.at[step],
            recv_sem=length_recv.at[step],
            device_id={"replica": lax.rem(me + step, groups)},
            device_id_type=MESH,
        )

    def q_copy(group, k, way):
        dest = z + (1 if way == 0 else -1)
        return pltpu.make_async_remote_copy(
            src_ref=qall.at[group, k],
            dst_ref=qall.at[group, k],
            send_sem=q_send.at[way, group, k],
            recv_sem=q_recv.at[group, k],
            device_id={"replica": dest * inner + x},
            device_id_type=MESH,
        )

    def page_copy(step, group, k):
        return pltpu.make_async_remote_copy(
            src_ref=outgoing.at[step - 1, group, k],
            dst_ref=arrived.at[step - 1, group, k],
            send_sem=page_send.at[step - 1, group, k],
            recv_sem=page_recv.at[step - 1, group, k],
            device_id={"replica": z * inner + lax.rem(x + step, inner)},
            device_id_type=MESH,
        )

    def back_copy(group, k, source):
        return pltpu.make_async_remote_copy(
            src_ref=back.at[group, k],
            dst_ref=came.at[source, k],
            send_sem=back_send.at[group, k],
            recv_sem=back_recv.at[source, k],
            device_id={"replica": group * inner + x},
            device_id_type=MESH,
        )

    def log_copy(group, k, source):
        return pltpu.make_async_remote_copy(
            src_ref=back_log.at[group, k],
            dst_ref=came_log.at[source, k],
            send_sem=log_send.at[group, k],
            recv_sem=log_recv.at[source, k],
            device_id={"replica": group * inner + x},
            device_id_type=MESH,
        )

    def weight_copy(index):
        return pltpu.make_async_copy(
            weight.at[:, pl.ds(pl.multiple_of(index * tile, tile), tile)],
            wbuf.at[index],
            weight_sem.at[index],
        )

    def core_copy(index):
        return pltpu.make_async_remote_copy(
            src_ref=part.at[index, 1 - core],
            dst_ref=sibling.at[index],
            send_sem=core_send.at[index],
            recv_sem=core_recv.at[index],
            device_id={"tensor": chip * CORES + 1 - core},
            device_id_type=MESH,
        )

    def part_copy(index, step):
        dest = lax.rem(chip + step, chips)
        return pltpu.make_async_remote_copy(
            src_ref=joined.at[index, step - 1],
            dst_ref=landed.at[index, step - 1],
            send_sem=part_send.at[index, step - 1],
            recv_sem=part_recv.at[index, step - 1],
            device_id={"tensor": dest * CORES + core},
            device_id_type=MESH,
        )

    perm[...] = selection(block, kv_count)

    side = z // half

    def served(turn):
        across = (1 - side) * (half + turn) + side * (half - 1 - turn)
        beside = side * half + lax.rem(z - side * half + 1 + turn - half + outer, half)
        far = (turn < half).astype(jnp.int32) if not isinstance(turn, int) else int(turn < half)
        return far * across + (1 - far) * beside

    loads[0].wait()
    loads[1].wait()
    pl.semaphore_wait(barrier, groups + shards - 2)
    for step in sorted(range(1, groups), key=lambda d: -min(d, groups - d)):
        table_copy(step).start()
        length_copy(step).start()
    for copy in q_loads:
        copy.wait()
    for k in range(kv_count):
        @pl.when(z < outer - 1)
        def _():
            q_copy(z, k, 0).start()

        @pl.when(z > 0)
        def _():
            q_copy(z, k, 1).start()

    loads[2].wait()
    loads[3].wait()

    def request(group, owner):
        count = jnp.int32(0)
        zero = jnp.int32(0)
        shelf, dialog, fill = [zero] * SLOT, [zero] * SLOT, [zero] * SLOT
        low = owner * pool_size
        for d in range(dialogs):
            total = length[group, d]
            for e in range(entries):
                place = table[group, d, e] - low
                live = jnp.minimum(total - e * PAGE, PAGE)
                hit = (place >= 0) & (place < pool_size) & (live > 0)
                for s in range(SLOT):
                    here = hit & (count == s)
                    shelf[s] = jnp.where(here, place, shelf[s])
                    dialog[s] = jnp.where(here, d, dialog[s])
                    fill[s] = jnp.where(here, live, fill[s])
                count = count + hit.astype(jnp.int32)
        return shelf, dialog, fill

    def await_tables(group):
        for other in range(inner):
            source = group * inner + other
            step = lax.rem(me - source + groups, groups)

            @pl.when(source != me)
            def _():
                table_copy(step).wait_recv()
                length_copy(step).wait_recv()

    def separate(shelf, put):
        for s in range(SLOT):
            for b in range(page_rows // block):
                split = jnp.dot(
                    perm[...],
                    pool_ref[shelf[s], b * block : (b + 1) * block, :],
                    preferred_element_type=jnp.float32,
                ).astype(jnp.bfloat16)
                for k in range(kv_count):
                    for kind in range(2):
                        low = (2 * k + kind) * block_tokens
                        put(k, s, kind, b * block_tokens, split[low : low + block_tokens])

    def relay(distance, k):
        @pl.when(z >= distance)
        def _():
            q_copy(z - distance, k, 0).wait_recv()

        @pl.when((z >= distance) & (z < outer - 1))
        def _():
            q_copy(z - distance, k, 0).start()

        @pl.when(z < outer - distance)
        def _():
            q_copy(z + distance, k, 1).wait_recv()

        @pl.when((z < outer - distance) & (z > 0))
        def _():
            q_copy(z + distance, k, 1).start()

    def send_pages(turn, carry):
        group = served(turn)
        await_tables(group)
        for step in range(1, inner):
            shelf, _, _ = request(group * inner + lax.rem(x + step, inner), me)

            def put(k, s, kind, at, rows_of):
                outgoing[step - 1, group, k, s, kind, at : at + block_tokens, :] = rows_of

            separate(shelf, put)
            for k in range(kv_count):
                page_copy(step, group, k).start()
        return carry

    lax.fori_loop(0, 1, send_pages, 0)
    for distance in range(1, half):
        relay(distance, 0)
    lax.fori_loop(1, outer, send_pages, 0)

    for index in range(tiles):
        weight_copy(index).start()

    def list_pages(group, carry):
        for step in range(inner):
            shelf, dialog, fill = request(
                group * inner + x, z * inner + lax.rem(x - step + inner, inner)
            )
            for s in range(SLOT):
                listed[group, step, s, 0] = dialog[s]
                listed[group, step, s, 1] = fill[s]
            if step == 0:

                def put(k, s, kind, at, rows_of):
                    kept[group, k, s, kind, at : at + block_tokens, :] = rows_of

                separate(shelf, put)
        return carry

    lax.fori_loop(0, half, list_pages, 0)
    for k in range(1, kv_count):
        for distance in range(1, half):
            relay(distance, k)
    lax.fori_loop(half, outer, list_pages, 0)

    fresh_rows = fresh_ref.shape[0]
    split = jnp.dot(
        selection(fresh_rows, kv_count), fresh_ref[...], preferred_element_type=jnp.float32
    ).astype(jnp.bfloat16)
    row_token = lax.broadcasted_iota(jnp.int32, (rows, token_rows), 0) % new_len
    col_token = lax.broadcasted_iota(jnp.int32, (rows, token_rows), 1)
    for k in range(kv_count):
        keys = split[(2 * k) * token_rows : (2 * k + 1) * token_rows]
        values = split[(2 * k + 1) * token_rows : (2 * k + 2) * token_rows]
        for d in range(dialogs):
            scores = lax.dot_general(
                qall[z, k, d], keys, CONTRACT, preferred_element_type=jnp.float32
            ) * scale
            causal = (col_token // new_len == d) & (col_token - d * new_len <= row_token)
            scores = jnp.where(causal, scores, floor_value)
            peak = jnp.max(scores, axis=-1, keepdims=True)
            weights = jnp.exp2(scores - peak).astype(jnp.bfloat16)
            peak_ref[z, k, d] = jnp.broadcast_to(peak, (rows, HD))
            amount_ref[z, k, d] = jnp.broadcast_to(
                jnp.sum(weights.astype(jnp.float32), axis=-1, keepdims=True), (rows, HD)
            )
            summed_ref[z, k, d] = jnp.dot(weights, values, preferred_element_type=jnp.float32)

    def absorb(group, k, step, pages, first):
        position = lax.broadcasted_iota(jnp.int32, (rows, PAGE), 1)
        dialog = [listed[group, step, s, 0] for s in range(SLOT)]
        fill = [listed[group, step, s, 1] for s in range(SLOT)]
        owned = [
            [jnp.broadcast_to(dialog[s], (rows, HD)) == d for d in range(dialogs)]
            for s in range(SLOT)
        ]
        for d in range(dialogs):
            qcur[d] = qall[group, k, d]
        scores, highs = [], []
        for s in range(SLOT):
            found = lax.dot_general(
                qcur[dialog[s]], pages[s, 0], CONTRACT, preferred_element_type=jnp.float32
            ) * scale
            found = jnp.where(position < fill[s], found, floor_value)
            scores.append(found)
            highs.append(jnp.broadcast_to(jnp.max(found, axis=-1, keepdims=True), (rows, HD)))
        peaks, keeps = [], []
        for d in range(dialogs):
            peak = functools.reduce(
                jnp.maximum,
                [jnp.where(owned[s][d], highs[s], floor_value) for s in range(SLOT)],
            )
            if not first:
                before = peak_ref[group, k, d]
                peak = jnp.maximum(peak, before)
                keeps.append(jnp.exp2(before - peak))
            peaks.append(peak)
            peak_ref[group, k, d] = peak
        amounts, sums = [], []
        for s in range(SLOT):
            peak = peaks[-1]
            for d in reversed(range(dialogs - 1)):
                peak = jnp.where(owned[s][d], peaks[d], peak)
            weights = jnp.exp2(scores[s] - peak).astype(jnp.bfloat16)
            amounts.append(
                jnp.broadcast_to(
                    jnp.sum(weights.astype(jnp.float32), axis=-1, keepdims=True), (rows, HD)
                )
            )
            sums.append(jnp.dot(weights, pages[s, 1], preferred_element_type=jnp.float32))
        for d in range(dialogs):
            amount = functools.reduce(
                jnp.add, [jnp.where(owned[s][d], amounts[s], 0.0) for s in range(SLOT)]
            )
            total = functools.reduce(
                jnp.add, [jnp.where(owned[s][d], sums[s], 0.0) for s in range(SLOT)]
            )
            if not first:
                amount = amount + keeps[d] * amount_ref[group, k, d]
                total = total + keeps[d] * summed_ref[group, k, d]
            amount_ref[group, k, d] = amount
            summed_ref[group, k, d] = total

    def absorb_kept(group, k, first):
        absorb(group, k, 0, kept.at[group, k], first)

    def absorb_arrived(group, k):
        for step in range(1, inner):
            page_copy(step, group, k).wait_recv()
            absorb(group, k, step, arrived.at[step - 1, group, k], False)

    def begin(k, carry):
        absorb_kept(z, k, False)
        return carry

    lax.fori_loop(0, kv_count, begin, 0)

    def serve(index, carry):
        group = served(index // kv_count)
        k = index % kv_count
        absorb_kept(group, k, True)
        absorb_arrived(group, k)
        for d in range(dialogs):
            amount = jnp.maximum(amount_ref[group, k, d], tiny_value)
            back[group, k, d] = (summed_ref[group, k, d] / amount).astype(jnp.bfloat16)
            log = peak_ref[group, k, d] + jnp.log2(amount)
            back_log[group, k, d : d + 1, :] = jnp.transpose(log)[:1]
        back_copy(group, k, z).start()
        log_copy(group, k, z).start()
        return carry

    def serve_far(index, carry):
        relay(half + index // kv_count, index % kv_count)
        return serve(index, carry)

    lax.fori_loop(0, half * kv_count, serve_far, 0)
    lax.fori_loop(half * kv_count, (outer - 1) * kv_count, serve, 0)

    def merge(turn, k):
        source = served(turn)
        back_copy(source, k, source).wait_recv()
        log_copy(source, k, source).wait_recv()
        for d in range(dialogs):
            line = came_log[source, k, d : d + 1, :]
            log = jnp.transpose(jnp.broadcast_to(line, (HD, rows)))
            before = peak_ref[z, k, d]
            peak = jnp.maximum(before, log)
            keep = jnp.exp2(before - peak)
            take = jnp.exp2(log - peak)
            peak_ref[z, k, d] = peak
            amount_ref[z, k, d] = keep * amount_ref[z, k, d] + take
            summed_ref[z, k, d] = keep * summed_ref[z, k, d] + take * came[
                source, k, d
            ].astype(jnp.float32)
        return k

    head_depth = per_group * HD
    batch = math.gcd(tiles, BATCH)

    def complete(k, carry):
        lax.fori_loop(0, half, merge, k)
        absorb_arrived(z, k)
        lax.fori_loop(half, outer - 1, merge, k)
        for d in range(dialogs):
            ratio = (summed_ref[z, k, d] / amount_ref[z, k, d]).astype(jnp.bfloat16)
            for g in range(per_group):
                attended[k, d * new_len : (d + 1) * new_len, g * HD : (g + 1) * HD] = ratio[
                    g * new_len : (g + 1) * new_len
                ]
        return carry

    def product_of(k, index):
        return jnp.dot(
            attended[k],
            wbuf[index, pl.ds(k * head_depth, head_depth), :],
            preferred_element_type=jnp.float32,
        )

    for k in range(kv_count):
        complete(k, 0)
        if k == kv_count - 1:
            break

        def collect(turn, carry):
            for offset in range(batch):
                index = turn * batch + offset
                if k == 0:
                    weight_copy(index).wait()
                    gathered[index] = product_of(k, index)
                else:
                    gathered[index] += product_of(k, index)
            return carry

        lax.fori_loop(0, tiles // batch, collect, 0)

    def join(index):
        core_copy(index).wait_recv()
        for step in range(1, chips):
            dest = lax.rem(chip + step, chips)
            total = part[index, core, dest].astype(jnp.float32) + sibling[index, dest].astype(
                jnp.float32
            )
            joined[index, step - 1] = total.astype(jnp.bfloat16)
            part_copy(index, step).start()

    def project(index, carry):
        if kv_count == 1:
            weight_copy(index).wait()
        product = product_of(kv_count - 1, index)
        if kv_count > 1:
            product = product + gathered[index]
        product = product.astype(jnp.bfloat16)
        for dest in range(shards):
            part[index, dest % CORES, dest // CORES] = product[
                dest * block_rows : (dest + 1) * block_rows
            ]
        core_copy(index).start()

        @pl.when(index >= LAG)
        def _():
            join(index - LAG)

        return carry

    lax.fori_loop(0, tiles, project, 0)

    def join_rest(index, carry):
        join(index)
        return carry

    lax.fori_loop(max(tiles - LAG, 0), tiles, join_rest, 0)

    def out_copy(index):
        return pltpu.make_async_copy(
            result.at[index],
            out_ref.at[:, pl.ds(pl.multiple_of(index * tile, tile), tile)],
            out_sem.at[index],
        )

    def finish(index, carry):
        total = part[index, core, chip].astype(jnp.float32) + sibling[index, chip].astype(
            jnp.float32
        )
        for step in range(1, chips):
            part_copy(index, step).wait_recv()
            total = total + landed[index, step - 1].astype(jnp.float32)
        result[index] = total.astype(out_ref.dtype)
        out_copy(index).start()
        return carry

    lax.fori_loop(0, tiles, finish, 0)

    def drain(index, carry):
        out_copy(index).wait()
        core_copy(index).wait_send()
        for step in range(1, chips):
            part_copy(index, step).wait_send()
        return carry

    lax.fori_loop(0, tiles, drain, 0)

    def drain_back(turn, carry):
        for k in range(kv_count):
            back_copy(served(turn), k, z).wait_send()
            log_copy(served(turn), k, z).wait_send()
        return carry

    lax.fori_loop(0, outer - 1, drain_back, 0)

    def drain_line(group, carry):
        for k in range(kv_count):
            for step in range(1, inner):
                page_copy(step, group, k).wait_send()

            @pl.when((group <= z) & (z < outer - 1))
            def _():
                q_copy(group, k, 0).wait_send()

            @pl.when((group >= z) & (z > 0))
            def _():
                q_copy(group, k, 1).wait_send()

        return carry

    lax.fori_loop(0, outer, drain_line, 0)
    for step in range(1, groups):
        table_copy(step).wait_send()
        length_copy(step).wait_send()


def local(queries, kv_new, pool, page_table, hist_len, o_weight):
    groups = lax.axis_size("replica")
    shards = lax.axis_size("tensor")
    outer, inner = spread(groups)
    pool_size, page_len, _, kv_width = pool.shape
    dialogs, entries = page_table.shape
    token_rows = queries.shape[0]
    new_len = token_rows // dialogs
    kv_count = kv_width // HD
    per_group = queries.shape[1] // kv_width
    rows = per_group * new_len
    depth, model = o_weight.shape
    tile = min(TILE, model)
    tiles = model // tile
    block_rows = token_rows // shards
    chips = shards // CORES
    page_rows = 2 * kv_count * page_len
    block = 256
    pages = pool.reshape(pool_size, page_len, 2, kv_count, HD).transpose(0, 1, 3, 2, 4)
    pages = pages.reshape(pool_size, page_rows, HD)
    fresh = kv_new.reshape(token_rows, 2, kv_count, HD).transpose(0, 2, 1, 3)
    fresh = fresh.reshape(2 * kv_count * token_rows, HD)
    anywhere = pl.BlockSpec(memory_space=pl.ANY)
    dma = pltpu.SemaphoreType.DMA
    bf16, f32 = jnp.bfloat16, jnp.float32
    return pl.pallas_call(
        functools.partial(kernel, groups, shards),
        out_shape=jax.ShapeDtypeStruct((block_rows, model), jnp.bfloat16),
        in_specs=[anywhere] * 6,
        out_specs=anywhere,
        scratch_shapes=[
            pltpu.SMEM((groups, dialogs, entries), jnp.int32),
            pltpu.SMEM((groups, dialogs), jnp.int32),
            pltpu.SMEM((outer, inner, SLOT, 2), jnp.int32),
            pltpu.VMEM((pool_size, page_rows, HD), bf16),
            pltpu.VMEM((2 * kv_count * token_rows, HD), bf16),
            pltpu.VMEM((outer, kv_count, SLOT, 2, page_len, HD), bf16),
            pltpu.VMEM((inner - 1, outer, kv_count, SLOT, 2, page_len, HD), bf16),
            pltpu.VMEM((inner - 1, outer, kv_count, SLOT, 2, page_len, HD), bf16),
            pltpu.VMEM((tiles, depth, tile), bf16),
            pltpu.VMEM((block, block), bf16),
            pltpu.VMEM((outer, kv_count, dialogs, rows, HD), bf16),
            pltpu.VMEM((dialogs, rows, HD), bf16),
            pltpu.VMEM((outer, kv_count, dialogs, rows, HD), f32),
            pltpu.VMEM((outer, kv_count, dialogs, rows, HD), f32),
            pltpu.VMEM((outer, kv_count, dialogs, rows, HD), f32),
            pltpu.VMEM((outer, kv_count, dialogs, rows, HD), bf16),
            pltpu.VMEM((outer, kv_count, dialogs, rows), f32),
            pltpu.VMEM((outer, kv_count, dialogs, rows, HD), bf16),
            pltpu.VMEM((outer, kv_count, dialogs, rows), f32),
            pltpu.VMEM((kv_count, token_rows, depth // kv_count), bf16),
            pltpu.VMEM((tiles, token_rows, tile), f32),
            pltpu.VMEM((tiles, CORES, chips, block_rows, tile), bf16),
            pltpu.VMEM((tiles, chips, block_rows, tile), bf16),
            pltpu.VMEM((tiles, chips - 1, block_rows, tile), bf16),
            pltpu.VMEM((tiles, chips - 1, block_rows, tile), bf16),
            pltpu.VMEM((tiles, block_rows, tile), bf16),
            dma((4,)),
            dma((kv_count, dialogs, per_group)),
            dma((tiles,)),
            dma((tiles,)),
            dma((groups,)),
            dma((groups,)),
            dma((groups,)),
            dma((groups,)),
            dma((2, outer, kv_count)),
            dma((outer, kv_count)),
            dma((inner - 1, outer, kv_count)),
            dma((inner - 1, outer, kv_count)),
            dma((outer, kv_count)),
            dma((outer, kv_count)),
            dma((outer, kv_count)),
            dma((outer, kv_count)),
            dma((tiles,)),
            dma((tiles,)),
            dma((tiles, chips - 1)),
            dma((tiles, chips - 1)),
        ],
        compiler_params=pltpu.CompilerParams(
            collective_id=0, has_side_effects=True, vmem_limit_bytes=63 * 1024 * 1024
        ),
        name="attend",
    )(queries, fresh, pages, page_table, hist_len, o_weight)


def solution(mesh):
    in_specs = (
        P("replica", "tensor"),
        P("replica", None, "tensor"),
        P("replica", None, None, "tensor"),
        P("replica", None),
        P("replica"),
        P("tensor", None),
    )
    out_specs = P(("replica", "tensor"), None)
    return jax.shard_map(local, mesh=mesh, in_specs=in_specs, out_specs=out_specs, check_vma=False)
```
